32 devices in a mesh: xy: 8 (over y, x, core), gz: 4 (over z).
Axes of the slice: x: 2, y: 2, z: 4, core: 2. Of those that a mesh axis runs over, the one named last changes fastest.
Arguments:
- field: float32 [64, 2, 3, 64, 256], P('gz', None, None, 'xy'), may hold values from -6 to 6
- source: float32 [64, 2, 3, 64, 256], P('gz', None, None, 'xy'), may hold values from -6 to 6
- classes: int32 [64, 64, 256], P('gz', 'xy'), may hold values from 0 to 15
- boundary: int32 [64, 64, 256], P('gz', 'xy'), may hold values 0 or 1
- conductance: float32 [16], replicated, may hold values from 0.001 to 1
- angles: float32 [3], replicated, may hold values from -3.140625 to 3.140625
- strengths: float32 [3], replicated, may hold values from 0.5 to 2
Outputs:
- relaxed: float32 [64, 2, 3, 64, 256], P('gz', None, None, 'xy')
The draws below stay inside these ranges and needn't reach their ends.
All inputs are finite; a program needn't handle non-finite values. No bound on the sum of `boundary` on one device may be relied on, other than what follows from the above.
Results may differ from the reference program's by a relative error of at most 0.00029.
Values sent between devices are 32-bit elements; how exact they have to be, the bound alone decides.
A program may use at most 64 MiB of HBM per device.

```python
import math
import jax
import jax.numpy as jnp
from jax import lax

NX = 256
CLASSES = 16
SWEEPS = 2
NZ = 64
NY = 64


def touch_ends(array, stream_key, least, largest):
    extent = array.shape
    place = [jax.random.randint(jax.random.fold_in(stream_key, axis), (), 0, extent[axis]) for axis in range(len(extent))]
    array = array.at[tuple(place)].set(least)
    longest = extent.index(max(extent))
    place[longest] = (place[longest] + 1) % extent[longest]
    return array.at[tuple(place)].set(largest)


def block_levels(rng, dims, pieces, least, largest):
    def one(position, blocks):
        steps = jax.random.uniform(jax.random.fold_in(jax.random.fold_in(rng, 6), position), (blocks,), jnp.float32, least / len(pieces), largest / len(pieces))
        return jnp.repeat(jnp.exp(steps), dims[position] // blocks).reshape((-1,) + (1,) * (len(dims) - position - 1))

    loudness = one(*pieces[0])
    for cut in pieces[1:]:
        loudness = loudness * one(*cut)
    return loudness


def scatter_about(key, extent, width, limit, split=(), kind=jnp.bfloat16):
    gain = block_levels(key, extent, split, -0.22, 0.18) if split else 1.0
    values = jax.random.normal(key, extent, jnp.float32) * width * gain
    return jnp.minimum(jnp.maximum(values, -limit), limit).astype(kind)


def setup_inputs(seed: int = 0) -> dict:
    keys = jax.random.split(jax.random.key(seed), 8)
    return {
        "field": scatter_about(keys[0], (NZ, 2, 3, NY, NX), 1.0, 6.0, ((0, 4), (3, 8)), jnp.float32),
        "source": scatter_about(keys[1], (NZ, 2, 3, NY, NX), 1.0, 6.0, ((0, 4), (3, 8)), jnp.float32),
        "classes": touch_ends(jax.random.randint(keys[2], (NZ, NY, NX), 0, CLASSES), jax.random.fold_in(keys[2], 1), 0, CLASSES - 1).astype(jnp.int32),
        "boundary": touch_ends((jax.random.randint(keys[3], (NZ, NY, NX), 0, 8) < 1).astype(jnp.int32), jax.random.fold_in(keys[3], 1), 0, 1),
        "conductance": jnp.clip(jnp.exp(jax.random.uniform(keys[4], (CLASSES,), jnp.float32, math.log(0.001), math.log(1.0))), 0.001, 1.0),
        "angles": jnp.clip(jax.random.uniform(keys[5], (3,), jnp.float32, -3.140625, 3.140625), -3.140625, 3.140625),
        "strengths": jnp.clip(jnp.exp(jax.random.uniform(keys[6], (3,), jnp.float32, math.log(0.5), math.log(2.0))), 0.5, 2.0),
    }


coupling = 0.1
penalty = 4.0


def about_depth(cosine, sine_val):
    filler = jnp.zeros_like(cosine)
    ones_fill = jnp.ones_like(cosine)
    return jnp.stack([jnp.stack([cosine, -sine_val, filler]), jnp.stack([sine_val, cosine, filler]), jnp.stack([filler, filler, ones_fill])])


def about_north(cosine, sine_val):
    filler = jnp.zeros_like(cosine)
    ones_fill = jnp.ones_like(cosine)
    return jnp.stack([jnp.stack([cosine, filler, sine_val]), jnp.stack([filler, ones_fill, filler]), jnp.stack([-sine_val, filler, cosine])])


def rotation(angles):
    cosines = jnp.cos(angles)
    sines = jnp.sin(angles)
    first = jnp.dot(about_depth(cosines[0], sines[0]), about_north(cosines[1], sines[1]), precision=lax.Precision.HIGHEST)
    return jnp.dot(first, about_depth(cosines[2], sines[2]), precision=lax.Precision.HIGHEST)


def sweep_forward(driven, diag_real, diag_imag, start):
    def advance(previous, slices):
        inverse, earlier = previous
        forcing, diag_re, diag_im = slices
        pivot_re = diag_re[None] - inverse[0]
        pivot_im = diag_im - inverse[1]
        weight_sq = 1.0 / (pivot_re * pivot_re + pivot_im * pivot_im)
        new_inverse = jnp.stack([pivot_re * weight_sq, -pivot_im * weight_sq])
        new_earlier = jnp.stack([forcing[0] + inverse[0] * earlier[0] - inverse[1] * earlier[1],
                                 forcing[1] + inverse[0] * earlier[1] + inverse[1] * earlier[0]])
        return (new_inverse, new_earlier), (new_inverse, new_earlier)

    last_state, history = lax.scan(advance, start, (driven, diag_real, diag_imag))
    return history


def sweep_backward(inverse_all, carried_all, start):
    def advance(following, slices):
        inverse, carried = slices
        summed = carried + following
        result = jnp.stack([inverse[0] * summed[0] - inverse[1] * summed[1],
                            inverse[0] * summed[1] + inverse[1] * summed[0]])
        return result, result

    last_state, history = lax.scan(advance, start, (inverse_all, carried_all), reverse=True)
    return history


def reference(field, source, classes, boundary, conductance, angles, strengths):
    rotation_matrix = rotation(angles)
    diag_real = 2.0 + 4.0 * coupling + penalty * boundary.astype(jnp.float32)
    diag_imag = conductance[classes][:, None] * strengths[None, :, None, None]
    current = field
    for repeat in range(SWEEPS):
        padded = jnp.pad(current, ((0, 0), (0, 0), (0, 0), (1, 1), (1, 1)))
        beside = padded[:, :, :, 2:, 1:-1] + padded[:, :, :, :-2, 1:-1] + padded[:, :, :, 1:-1, 2:] + padded[:, :, :, 1:-1, :-2]
        driven = source + coupling * beside
        turned = jnp.einsum('cj,zpcyx->zpjyx', rotation_matrix, driven, precision=lax.Precision.HIGHEST)
        blank = jnp.zeros(turned.shape[1:], jnp.float32)
        inverse_all, carried_all = sweep_forward(turned, diag_real, diag_imag, (blank, blank))
        solved = sweep_backward(inverse_all, carried_all, blank)
        current = jnp.einsum('cj,zpjyx->zpcyx', rotation_matrix, solved, precision=lax.Precision.HIGHEST)
    return current
```

```python
import functools

import jax
import jax.numpy as jnp
from jax import lax
from jax.experimental import pallas as pl
from jax.experimental.pallas import tpu as pltpu
from jax.sharding import PartitionSpec as P

SWEEPS = 2
PIECES = 2

coupling = 0.1
penalty = 4.0


def mul(a, b):
    return (a[0] * b[0] - a[1] * b[1], a[0] * b[1] + a[1] * b[0])


def add(a, b):
    return (a[0] + b[0], a[1] + b[1])


def inv(a):
    weight = 1.0 / (a[0] * a[0] + a[1] * a[1])
    return (a[0] * weight, -a[1] * weight)


def one_minus(a):
    return (1.0 - a[0], -a[1])


def get(ref, *at):
    return (ref[at + (0,)], ref[at + (1,)])


def put(ref, value, *at):
    ref[at + (0,)] = value[0]
    ref[at + (1,)] = value[1]


def rotation(angles, shape):
    cos = [jnp.cos(jnp.full(shape, angles[i], jnp.float32)) for i in range(3)]
    sin = [jnp.sin(jnp.full(shape, angles[i], jnp.float32)) for i in range(3)]
    (ca, cb, cc), (sa, sb, sc) = cos, sin
    left = [[ca * cb, -sa, ca * sb], [sa * cb, ca, sa * sb], [-sb, jnp.zeros_like(cb), cb]]
    return [[row[0] * cc + row[1] * sc, row[1] * cc - row[0] * sc, row[2]] for row in left]


def relax(
    ngz,
    nxy,
    field,
    source,
    classes,
    boundary,
    conductance,
    angles,
    strengths,
    out,
    U,
    S,
    C,
    B,
    SG,
    DR,
    PH,
    PHI,
    PSI,
    T,
    OUT,
    QM,
    ends,
    coef,
    near,
    halo_out,
    halo_in,
    lam_in,
    lam_out,
    ch_in,
    ch_out,
    in_sems,
    out_sems,
    halo_send,
    halo_recv,
    lam_send,
    lam_recv,
    ch_send,
    ch_recv,
):
    ix, iz = lax.axis_index("xy"), lax.axis_index("gz")
    depth, _, _, rows, width = U.shape
    kinds = conductance.shape[0]
    plane = (rows, width)
    has = {
        ("xy", 0): ix > 0,
        ("xy", 1): ix < nxy - 1,
        ("gz", 0): iz > 0,
        ("gz", 1): iz < ngz - 1,
    }
    where_is = {
        ("xy", 0): ix - 1,
        ("xy", 1): ix + 1,
        ("gz", 0): iz - 1,
        ("gz", 1): iz + 1,
    }
    loads = [
        pltpu.make_async_copy(src, dst, in_sems.at[i])
        for i, (src, dst) in enumerate(((field, U), (classes, C), (boundary, B), (source, S)))
    ]
    for load in loads:
        load.start()

    barrier = pltpu.get_barrier_semaphore()
    for key, there in has.items():

        @pl.when(there)
        def _():
            pl.semaphore_signal(
                barrier,
                inc=1,
                device_id={key[0]: where_is[key]},
                device_id_type=pl.DeviceIdType.MESH,
            )

    count = sum(there.astype(jnp.int32) for there in has.values())
    pl.semaphore_wait(barrier, count)

    def remote(src, dst, send, recv, key):
        return pltpu.make_async_remote_copy(
            src_ref=src,
            dst_ref=dst,
            send_sem=send,
            recv_sem=recv,
            device_id={key[0]: where_is[key]},
            device_id_type=pl.DeviceIdType.MESH,
        )

    zs = depth // PIECES
    lines = zs * 6

    def halo_copy(sweep, side, piece):
        span = pl.ds(piece * lines, lines)
        return remote(
            halo_out.at[sweep, side, span],
            halo_in.at[sweep, side, span],
            halo_send.at[sweep, side, piece],
            halo_recv.at[sweep, side, piece],
            ("xy", 1 - side),
        )

    def send_halo(sweep, piece):
        for side in range(2):

            @pl.when(has["xy", 1 - side])
            def _():
                halo_copy(sweep, side, piece).start()

    def pack(sweep, z, values):
        for i in range(6):
            halo_out[sweep, 0, pl.ds(z * 6 + i, 1), :] = values[i][rows - 1 :, :]
            halo_out[sweep, 1, pl.ds(z * 6 + i, 1), :] = values[i][:1, :]

    for side in range(2):

        @pl.when(jnp.logical_not(has["xy", side]))
        def _():
            for sweep in range(SWEEPS):
                halo_in[sweep, side] = jnp.zeros(halo_in.shape[2:], jnp.float32)

        @pl.when(jnp.logical_not(has["gz", side]))
        def _():
            lam_in[side] = jnp.zeros(lam_in.shape[1:], jnp.float32)
            for sweep in range(SWEEPS):
                for j in range(3):
                    ch_in[sweep, side, j] = jnp.zeros(ch_in.shape[3:], jnp.float32)

    loads[0].wait()
    for piece in range(PIECES):

        def pack_first(k, carry):
            z = piece * zs + k
            pack(0, z, [U[z, i // 3, i % 3] for i in range(6)])
            return carry

        lax.fori_loop(0, zs, pack_first, 0)
        send_halo(0, piece)

    loads[1].wait()
    loads[2].wait()

    def diagonal(z, carry):
        ids = C[z]
        sigma = jnp.zeros(plane, jnp.float32)
        for kind in range(kinds):
            sigma = jnp.where(ids == kind, conductance[kind], sigma)
        SG[z] = sigma
        DR[z] = 2.0 + 4.0 * coupling + penalty * B[z].astype(jnp.float32)
        return carry

    lax.fori_loop(0, depth, diagonal, 0)

    def diag(z):
        real = jnp.broadcast_to(DR[z][None], (3,) + plane)
        sigma = SG[z]
        return real, jnp.stack([sigma * strengths[j] for j in range(3)])

    none = (jnp.zeros((3,) + plane, jnp.float32),) * 2

    def pivots(k, carry):
        p, q = carry
        z, back = k, depth - 1 - k
        d, f = diag(z), diag(back)
        p = inv((d[0] - p[0], d[1] - p[1]))
        q = inv((f[0] - q[0], f[1] - q[1]))
        put(PH, p, z)
        put(PHI, q, back)
        return p, q

    lax.fori_loop(0, depth, pivots, (none, none))
    ones = (jnp.ones((3,) + plane, jnp.float32), none[0])

    def columns(k, carry):
        down, up = carry
        z, back = k, depth - 1 - k
        down = mul(get(PHI, z), down)
        up = mul(get(PH, back), up)
        put(PHI, down, z)
        put(PSI, up, back)
        return down, up

    lax.fori_loop(0, depth, columns, (ones, ones))
    LEFT, RIGHT = 0, 1
    tip = (lambda: get(PHI, 0), lambda: get(PSI, depth - 1))
    across = lambda: get(PSI, 0)

    def lam_copy(side):
        return remote(
            lam_out.at[side],
            lam_in.at[side],
            lam_send.at[side],
            lam_recv.at[side],
            ("gz", 1 - side),
        )

    def pass_lam(side):
        @pl.when(has["gz", side])
        def _():
            lam_copy(side).wait_recv()

        lam = get(lam_in, side)
        kappa = mul(across(), inv(one_minus(mul(tip[side](), lam))))
        both = mul(kappa, lam)
        put(coef, kappa, side)
        put(coef, both, 2 + side)
        put(lam_out, add(tip[1 - side](), mul(across(), both)), side)

        @pl.when(has["gz", 1 - side])
        def _():
            lam_copy(side).start()

    def chain_copy(sweep, side, j):
        return remote(
            ch_out.at[sweep, side, j],
            ch_in.at[sweep, side, j],
            ch_send.at[sweep, side, j],
            ch_recv.at[sweep, side, j],
            ("gz", 1 - side),
        )

    def pass_chain(sweep, side):
        for j in range(3):
            base = add(
                (ends[1 - side, 0, j], ends[1 - side, 1, j]),
                mul(
                    (coef[2 + side, 0, j], coef[2 + side, 1, j]),
                    (ends[side, 0, j], ends[side, 1, j]),
                ),
            )

            @pl.when(has["gz", side])
            def _():
                chain_copy(sweep, side, j).wait_recv()

            result = add(
                base,
                mul(
                    (coef[side, 0, j], coef[side, 1, j]),
                    (ch_in[sweep, side, j, 0], ch_in[sweep, side, j, 1]),
                ),
            )
            ch_out[sweep, side, j, 0] = result[0]
            ch_out[sweep, side, j, 1] = result[1]

            @pl.when(has["gz", 1 - side])
            def _():
                chain_copy(sweep, side, j).start()

    left_first = iz * 2 < ngz - 1

    def near_side(run):
        @pl.when(left_first)
        def _():
            run(LEFT)

        @pl.when(jnp.logical_not(left_first))
        def _():
            run(RIGHT)

    def far_side(run):
        @pl.when(left_first)
        def _():
            run(RIGHT)

        @pl.when(jnp.logical_not(left_first))
        def _():
            run(LEFT)

    @pl.when(jnp.logical_not(has["gz", 0]))
    def _():
        pass_lam(LEFT)

    @pl.when(jnp.logical_not(has["gz", 1]))
    def _():
        pass_lam(RIGHT)

    angle_matrix = rotation(angles, (rows, 128))
    for c in range(3):
        for j in range(3):
            QM[c, j] = angle_matrix[c][j]

    def matrix():
        return [
            [jnp.concatenate([QM[c, j]] * (width // 128), axis=1) for j in range(3)]
            for c in range(3)
        ]

    row = lax.broadcasted_iota(jnp.int32, plane, 0)
    lane = lax.broadcasted_iota(jnp.int32, plane, 1)
    zero = jnp.zeros(plane, jnp.float32)

    def turn(q, driven):
        return [
            jnp.stack(
                [
                    q[0][j] * driven[p][0] + q[1][j] * driven[p][1] + q[2][j] * driven[p][2]
                    for j in range(3)
                ]
            )
            for p in range(2)
        ]

    def inner(z, carry):
        first, last = carry
        q = matrix()
        driven = []
        for p in range(2):
            of = []
            for c in range(3):
                u = U[z, p, c]
                beside = jnp.where(lane == 0, zero, pltpu.roll(u, 1, 1))
                beside += jnp.where(lane == width - 1, zero, pltpu.roll(u, width - 1, 1))
                beside += jnp.where(row == 0, zero, pltpu.roll(u, 1, 0))
                beside += jnp.where(row == rows - 1, zero, pltpu.roll(u, rows - 1, 0))
                of.append(S[z, p, c] + coupling * beside)
            driven.append(of)
        turned = turn(q, driven)
        put(T, turned, z)
        return add(first, mul(get(PHI, z), turned)), add(last, mul(get(PSI, z), turned))

    def outer(sweep, z, carry):
        first, last = carry
        q = matrix()
        driven = []
        for p in range(2):
            of = []
            for c in range(3):
                at = pl.ds(z * 6 + p * 3 + c, 1)
                above = jnp.broadcast_to(halo_in[sweep, 0, at, :], plane)
                below = jnp.broadcast_to(halo_in[sweep, 1, at, :], plane)
                edge = jnp.where(row == 0, above, zero) + jnp.where(row == rows - 1, below, zero)
                of.append(coupling * edge)
            driven.append(of)
        turned = turn(q, driven)
        put(T, add(get(T, z), turned), z)
        return add(first, mul(get(PHI, z), turned)), add(last, mul(get(PSI, z), turned))

    loads[3].wait()
    for sweep in range(SWEEPS):
        sums = lax.fori_loop(0, depth, inner, (none, none))
        for piece in range(PIECES):
            for side in range(2):

                @pl.when(has["xy", side])
                def _():
                    halo_copy(sweep, side, piece).wait_recv()

            sums = lax.fori_loop(
                piece * zs, (piece + 1) * zs, functools.partial(outer, sweep), sums
            )
        put(ends, sums[0], 0)
        put(ends, sums[1], 1)

        if sweep == 0:
            def late(side):
                @pl.when(has["gz", side])
                def _():
                    pass_lam(side)

            near_side(late)
            near_side(lambda side: pass_chain(0, side))
        else:
            near_side(lambda side: pass_chain(1, side))

        def forward(z, m):
            m = mul(get(PH, z), add(get(T, z), m))
            put(T, m, z)
            return m

        def backward(k, w):
            z = depth - 1 - k
            w = add(get(T, z), mul(get(PH, z), w))
            put(T, w, z)
            return w

        if sweep == 0:
            far_side(late)
        lax.fori_loop(0, depth, forward, none)
        lax.fori_loop(0, depth, backward, none)
        if sweep == 0:
            for side in range(2):
                lam, away = get(lam_in, side), get(lam_out, 1 - side)
                det = inv(one_minus(mul(lam, away)))
                put(coef, det, 6 + side)
                put(coef, mul(det, lam), 4 + side)
        far_side(functools.partial(pass_chain, sweep))

        for side in range(2):
            for j in range(3):
                arrived = (ch_in[sweep, side, j, 0], ch_in[sweep, side, j, 1])
                other = (ch_out[sweep, 1 - side, j, 0], ch_out[sweep, 1 - side, j, 1])
                value = add(
                    mul((coef[6 + side, 0, j], coef[6 + side, 1, j]), arrived),
                    mul((coef[4 + side, 0, j], coef[4 + side, 1, j]), other),
                )
                near[side, 0, j] = value[0]
                near[side, 1, j] = value[1]

        final = sweep == SWEEPS - 1

        def join(z, carry):
            q = matrix()
            before, after = get(near, 0), get(near, 1)
            w = add(add(get(T, z), mul(get(PHI, z), before)), mul(get(PSI, z), after))
            values = []
            for p in range(2):
                for c in range(3):
                    values.append(q[c][0] * w[p][0] + q[c][1] * w[p][1] + q[c][2] * w[p][2])
            target = OUT if final else U
            for i in range(6):
                target[z, i // 3, i % 3] = values[i]
            if not final:
                pack(sweep + 1, z, values)
            return carry

        for piece in range(PIECES):
            lax.fori_loop(piece * zs, (piece + 1) * zs, join, 0)
            if final:
                span = pl.ds(piece * zs, zs)
                pltpu.make_async_copy(OUT.at[span], out.at[span], out_sems.at[piece]).start()
            else:
                send_halo(sweep + 1, piece)

    for side in range(2):

        @pl.when(has["xy", 1 - side])
        def _():
            for sweep in range(SWEEPS):
                for piece in range(PIECES):
                    halo_copy(sweep, side, piece).wait_send()

        @pl.when(has["gz", 1 - side])
        def _():
            lam_copy(side).wait_send()
            for sweep in range(SWEEPS):
                for j in range(3):
                    chain_copy(sweep, side, j).wait_send()

    for piece in range(PIECES):
        span = pl.ds(piece * zs, zs)
        pltpu.make_async_copy(OUT.at[span], out.at[span], out_sems.at[piece]).wait()


def local(ngz, nxy, field, source, classes, boundary, conductance, angles, strengths):
    depth, _, _, rows, width = field.shape
    f32 = jnp.float32
    block = pltpu.VMEM(field.shape, f32)
    flat = (depth, rows, width)
    line = (2, 3, rows, width)
    dma = pltpu.SemaphoreType.DMA
    hbm = pl.BlockSpec(memory_space=pl.ANY)
    smem = pl.BlockSpec(memory_space=pltpu.SMEM)
    return pl.pallas_call(
        functools.partial(relax, ngz, nxy),
        out_shape=jax.ShapeDtypeStruct(field.shape, f32),
        in_specs=[hbm] * 4 + [smem] * 3,
        out_specs=hbm,
        scratch_shapes=[
            block,
            block,
            pltpu.VMEM(flat, jnp.int32),
            pltpu.VMEM(flat, jnp.int32),
            pltpu.VMEM(flat, f32),
            pltpu.VMEM(flat, f32),
            block,
            block,
            block,
            block,
            block,
            pltpu.VMEM((3, 3, rows, 128), f32),
            pltpu.VMEM((2,) + line, f32),
            pltpu.VMEM((8,) + line, f32),
            pltpu.VMEM((2,) + line, f32),
            pltpu.VMEM((SWEEPS, 2, depth * 6, width), f32),
            pltpu.VMEM((SWEEPS, 2, depth * 6, width), f32),
            pltpu.VMEM((2,) + line, f32),
            pltpu.VMEM((2,) + line, f32),
            pltpu.VMEM((SWEEPS, 2, 3, 2, rows, width), f32),
            pltpu.VMEM((SWEEPS, 2, 3, 2, rows, width), f32),
            dma((4,)),
            dma((PIECES,)),
            dma((SWEEPS, 2, PIECES)),
            dma((SWEEPS, 2, PIECES)),
            dma((2,)),
            dma((2,)),
            dma((SWEEPS, 2, 3)),
            dma((SWEEPS, 2, 3)),
        ],
        compiler_params=pltpu.CompilerParams(collective_id=0, has_side_effects=True),
    )(field, source, classes, boundary, conductance, angles, strengths)


def solution(mesh):
    in_specs = (
        P("gz", None, None, "xy", None),
        P("gz", None, None, "xy", None),
        P("gz", "xy", None),
        P("gz", "xy", None),
        P(),
        P(),
        P(),
    )
    out_specs = P("gz", None, None, "xy", None)
    body = functools.partial(local, mesh.shape["gz"], mesh.shape["xy"])
    return jax.shard_map(body, mesh=mesh, in_specs=in_specs, out_specs=out_specs, check_vma=False)
```

```python
import functools

import jax
import jax.numpy as jnp
from jax import lax
from jax.experimental import pallas as pl
from jax.experimental.pallas import tpu as pltpu
from jax.sharding import PartitionSpec as P

SWEEPS = 2
PIECES = 2

coupling = 0.1
penalty = 4.0


def mul(a, b):
    return (a[0] * b[0] - a[1] * b[1], a[0] * b[1] + a[1] * b[0])


def add(a, b):
    return (a[0] + b[0], a[1] + b[1])


def inv(a):
    weight = 1.0 / (a[0] * a[0] + a[1] * a[1])
    return (a[0] * weight, -a[1] * weight)


def one_minus(a):
    return (1.0 - a[0], -a[1])


def get(ref, *at):
    return (ref[at + (0,)], ref[at + (1,)])


def put(ref, value, *at):
    ref[at + (0,)] = value[0]
    ref[at + (1,)] = value[1]


def rotation(angles, shape):
    cos = [jnp.cos(jnp.full(shape, angles[i], jnp.float32)) for i in range(3)]
    sin = [jnp.sin(jnp.full(shape, angles[i], jnp.float32)) for i in range(3)]
    (ca, cb, cc), (sa, sb, sc) = cos, sin
    left = [[ca * cb, -sa, ca * sb], [sa * cb, ca, sa * sb], [-sb, jnp.zeros_like(cb), cb]]
    return [[row[0] * cc + row[1] * sc, row[1] * cc - row[0] * sc, row[2]] for row in left]


def relax(
    ngz,
    nxy,
    field,
    source,
    classes,
    boundary,
    conductance,
    angles,
    strengths,
    out,
    U,
    S,
    C,
    B,
    SG,
    DR,
    PH,
    PHI,
    PSI,
    T,
    OUT,
    QM,
    ends,
    coef,
    near,
    halo_out,
    halo_in,
    value_in,
    info_in,
    info_out,
    lam_in,
    lam_out,
    own_in,
    own_out,
    ch_in,
    ch_out,
    in_sems,
    out_sems,
    halo_send,
    halo_recv,
    info_send,
    info_recv,
    lam_send,
    lam_recv,
    own_send,
    own_recv,
    ch_send,
    ch_recv,
):
    ix, iz = lax.axis_index("xy"), lax.axis_index("gz")
    depth, _, _, rows, width = U.shape
    kinds = conductance.shape[0]
    plane = (rows, width)
    has = {
        ("xy", 0): ix > 0,
        ("xy", 1): ix < nxy - 1,
    }
    where_is = {
        ("xy", 0): ix - 1,
        ("xy", 1): ix + 1,
    }
    for steps in (1, 2):
        has["gz", -steps] = iz >= steps
        has["gz", steps] = iz < ngz - steps
        where_is["gz", -steps] = iz - steps
        where_is["gz", steps] = iz + steps

    loads = [
        pltpu.make_async_copy(src, dst, in_sems.at[i])
        for i, (src, dst) in enumerate(((field, U), (classes, C), (boundary, B), (source, S)))
    ]
    for load in loads:
        load.start()

    barrier = pltpu.get_barrier_semaphore()
    for key, there in has.items():

        @pl.when(there)
        def _():
            pl.semaphore_signal(
                barrier,
                inc=1,
                device_id={key[0]: where_is[key]},
                device_id_type=pl.DeviceIdType.MESH,
            )

    count = sum(there.astype(jnp.int32) for there in has.values())
    pl.semaphore_wait(barrier, count)

    def remote(src, dst, send, recv, key):
        return pltpu.make_async_remote_copy(
            src_ref=src,
            dst_ref=dst,
            send_sem=send,
            recv_sem=recv,
            device_id={key[0]: where_is[key]},
            device_id_type=pl.DeviceIdType.MESH,
        )

    zs = depth // PIECES
    lines = zs * 6

    def halo_copy(sweep, side, piece):
        span = pl.ds(piece * lines, lines)
        return remote(
            halo_out.at[sweep, side, span],
            halo_in.at[sweep, side, span],
            halo_send.at[sweep, side, piece],
            halo_recv.at[sweep, side, piece],
            ("xy", 1 - side),
        )

    def send_halo(sweep, piece):
        for side in range(2):

            @pl.when(has["xy", 1 - side])
            def _():
                halo_copy(sweep, side, piece).start()

    def pack(sweep, z, values):
        for i in range(6):
            halo_out[sweep, 0, pl.ds(z * 6 + i, 1), :] = values[i][rows - 1 :, :]
            halo_out[sweep, 1, pl.ds(z * 6 + i, 1), :] = values[i][:1, :]


    for side in range(2):

        @pl.when(jnp.logical_not(has["xy", side]))
        def _():
            for sweep in range(SWEEPS):
                halo_in[sweep, side] = jnp.zeros(halo_in.shape[2:], jnp.float32)

        @pl.when((iz if side == 0 else ngz - 1 - iz) < 2)
        def _():
            for part in range(3, 9):
                info_in[side, part] = jnp.zeros(info_in.shape[2:], jnp.float32)
            lam_in[side] = jnp.zeros(lam_in.shape[1:], jnp.float32)
            for sweep in range(SWEEPS):
                for j in range(3):
                    ch_in[sweep, side, j] = jnp.zeros(ch_in.shape[3:], jnp.float32)


    loads[0].wait()
    for piece in range(PIECES):

        def pack_first(k, carry):
            z = piece * zs + k
            pack(0, z, [U[z, i // 3, i % 3] for i in range(6)])
            return carry

        lax.fori_loop(0, zs, pack_first, 0)
        send_halo(0, piece)


    loads[1].wait()
    loads[2].wait()

    def diagonal(z, carry):
        ids = C[z]
        sigma = jnp.zeros(plane, jnp.float32)
        for kind in range(kinds):
            sigma = jnp.where(ids == kind, conductance[kind], sigma)
        SG[z] = sigma
        DR[z] = 2.0 + 4.0 * coupling + penalty * B[z].astype(jnp.float32)
        return carry

    lax.fori_loop(0, depth, diagonal, 0)

    def diag(z):
        real = jnp.broadcast_to(DR[z][None], (3,) + plane)
        sigma = SG[z]
        return real, jnp.stack([sigma * strengths[j] for j in range(3)])

    none = (jnp.zeros((3,) + plane, jnp.float32),) * 2

    def pivots(k, carry):
        p, q = carry
        z, back = k, depth - 1 - k
        d, f = diag(z), diag(back)
        p = inv((d[0] - p[0], d[1] - p[1]))
        q = inv((f[0] - q[0], f[1] - q[1]))
        put(PH, p, z)
        put(PHI, q, back)
        return p, q


    lax.fori_loop(0, depth, pivots, (none, none))
    ones = (jnp.ones((3,) + plane, jnp.float32), none[0])

    def columns(k, carry):
        down, up = carry
        z, back = k, depth - 1 - k
        down = mul(get(PHI, z), down)
        up = mul(get(PH, back), up)
        put(PHI, down, z)
        put(PSI, up, back)
        return down, up


    lax.fori_loop(0, depth, columns, (ones, ones))
    LEFT, RIGHT = 0, 1
    tip = (lambda: get(PHI, 0), lambda: get(PSI, depth - 1))
    across = lambda: get(PSI, 0)

    place = (iz, ngz - 1 - iz)
    even = [lax.rem(k, 2) == 0 for k in place]
    odd = [lax.rem(k, 2) == 1 for k in place]
    onward = [ngz - 1 - k for k in place]

    def to(side, steps):
        return {"gz": iz + steps if side == LEFT else iz - steps}

    def chain_copy(src, dst, send, recv, side, steps):
        return pltpu.make_async_remote_copy(
            src_ref=src,
            dst_ref=dst,
            send_sem=send,
            recv_sem=recv,
            device_id=to(side, steps),
            device_id_type=pl.DeviceIdType.MESH,
        )

    def info_copy(side, j):
        return chain_copy(
            info_out.at[side, j],
            info_in.at[side, j],
            info_send.at[side, j],
            info_recv.at[side, j],
            side,
            1,
        )

    def lam_copy(side, steps, j):
        return chain_copy(
            lam_out.at[side, j],
            lam_in.at[side, j],
            lam_send.at[side, steps - 1, j],
            lam_recv.at[side, j],
            side,
            steps,
        )

    def own_copy(sweep, side, j):
        return chain_copy(
            own_out.at[sweep, side, j],
            own_in.at[sweep, side, j],
            own_send.at[sweep, side, j],
            own_recv.at[sweep, side, j],
            side,
            1,
        )

    def x_copy(sweep, side, steps, j):
        return chain_copy(
            ch_out.at[sweep, side, j],
            ch_in.at[sweep, side, j],
            ch_send.at[sweep, side, steps - 1, j],
            ch_recv.at[sweep, side, j],
            side,
            steps,
        )

    both = jnp.logical_and

    def send_info(side):
        parts = (tip[1 - side](), tip[side](), across())
        for part in range(3):
            for j in range(3):
                for p in range(2):
                    info_out[side, part * 3 + j, p] = parts[part][p][j]
            sends = both(even[side], onward[side] >= 1)

            @pl.when(sends if part == 0 else both(sends, place[side] > 0))
            def _():
                for j in range(3):
                    info_copy(side, part * 3 + j).start()

    def pass_lam(side):
        @pl.when(odd[side])
        def _():
            for j in range(3):
                info_copy(side, j).wait_recv()

        @pl.when(both(odd[side], place[side] >= 2))
        def _():
            for j in range(3, 9):
                info_copy(side, j).wait_recv()

        @pl.when(place[side] >= 2)
        def _():
            for j in range(3):
                lam_copy(side, 1, j).wait_recv()

        for j in range(3):
            tips = [(info_in[side, 3 * k + j, 0], info_in[side, 3 * k + j, 1]) for k in range(3)]
            given = (lam_in[side, j, 0], lam_in[side, j, 1])

            @pl.when(odd[side])
            def _():
                skip = mul(tips[2], inv(one_minus(mul(tips[1], given))))
                lam = add(tips[0], mul(tips[2], mul(skip, given)))
                for p in range(2):
                    coef[8 + side, p, j] = skip[p]
                    coef[10 + side, p, j] = lam[p]

            @pl.when(even[side])
            def _():
                for p in range(2):
                    coef[10 + side, p, j] = given[p]

            of = lambda pair: (pair[0][j], pair[1][j])
            lam = (coef[10 + side, 0, j], coef[10 + side, 1, j])
            kappa = mul(of(across()), inv(one_minus(mul(of(tip[side]()), lam))))
            over = mul(kappa, lam)
            value = add(of(tip[1 - side]()), mul(of(across()), over))
            for p in range(2):
                coef[side, p, j] = kappa[p]
                coef[2 + side, p, j] = over[p]
                lam_out[side, j, p] = value[p]

            for steps in (2, 1):

                @pl.when(both(odd[side], onward[side] >= steps))
                def _():
                    lam_copy(side, steps, j).start()

    def own_sum(sweep, side):
        for j in range(3):
            base = add(
                (ends[1 - side, 0, j], ends[1 - side, 1, j]),
                mul(
                    (coef[2 + side, 0, j], coef[2 + side, 1, j]),
                    (ends[side, 0, j], ends[side, 1, j]),
                ),
            )
            for p in range(2):
                own_out[sweep, side, j, p] = base[p]

            @pl.when(both(even[side], onward[side] >= 1))
            def _():
                own_copy(sweep, side, j).start()

    def pass_chain(sweep, side):
        for j in range(3):

            @pl.when(odd[side])
            def _():
                own_copy(sweep, side, j).wait_recv()

            @pl.when(place[side] >= 2)
            def _():
                x_copy(sweep, side, 1, j).wait_recv()

            given = (ch_in[sweep, side, j, 0], ch_in[sweep, side, j, 1])

            @pl.when(odd[side])
            def _():
                own = (own_in[sweep, side, j, 0], own_in[sweep, side, j, 1])
                x = add(own, mul((coef[8 + side, 0, j], coef[8 + side, 1, j]), given))
                for p in range(2):
                    value_in[side, j, p] = x[p]

            @pl.when(even[side])
            def _():
                for p in range(2):
                    value_in[side, j, p] = given[p]

            x = (value_in[side, j, 0], value_in[side, j, 1])
            base = (own_out[sweep, side, j, 0], own_out[sweep, side, j, 1])
            result = add(base, mul((coef[side, 0, j], coef[side, 1, j]), x))
            for p in range(2):
                ch_out[sweep, side, j, p] = result[p]

            for steps in (2, 1):

                @pl.when(both(odd[side], onward[side] >= steps))
                def _():
                    x_copy(sweep, side, steps, j).start()

    left_first = iz * 2 < ngz - 1

    def near_side(run):
        @pl.when(left_first)
        def _():
            run(LEFT)

        @pl.when(jnp.logical_not(left_first))
        def _():
            run(RIGHT)

    def far_side(run):
        @pl.when(left_first)
        def _():
            run(RIGHT)

        @pl.when(jnp.logical_not(left_first))
        def _():
            run(LEFT)


    near_side(send_info)
    far_side(send_info)


    angle_matrix = rotation(angles, (rows, 128))
    for c in range(3):
        for j in range(3):
            QM[c, j] = angle_matrix[c][j]

    def matrix():
        return [
            [jnp.concatenate([QM[c, j]] * (width // 128), axis=1) for j in range(3)]
            for c in range(3)
        ]

    row = lax.broadcasted_iota(jnp.int32, plane, 0)
    lane = lax.broadcasted_iota(jnp.int32, plane, 1)
    zero = jnp.zeros(plane, jnp.float32)

    def turn(q, driven):
        return [
            jnp.stack(
                [
                    q[0][j] * driven[p][0] + q[1][j] * driven[p][1] + q[2][j] * driven[p][2]
                    for j in range(3)
                ]
            )
            for p in range(2)
        ]

    def inner(z, carry):
        first, last = carry
        q = matrix()
        driven = []
        for p in range(2):
            of = []
            for c in range(3):
                u = U[z, p, c]
                beside = jnp.where(lane == 0, zero, pltpu.roll(u, 1, 1))
                beside += jnp.where(lane == width - 1, zero, pltpu.roll(u, width - 1, 1))
                beside += jnp.where(row == 0, zero, pltpu.roll(u, 1, 0))
                beside += jnp.where(row == rows - 1, zero, pltpu.roll(u, rows - 1, 0))
                of.append(S[z, p, c] + coupling * beside)
            driven.append(of)
        turned = turn(q, driven)
        put(T, turned, z)
        return add(first, mul(get(PHI, z), turned)), add(last, mul(get(PSI, z), turned))

    def outer(sweep, z, carry):
        first, last = carry
        q = matrix()
        driven = []
        for p in range(2):
            of = []
            for c in range(3):
                at = pl.ds(z * 6 + p * 3 + c, 1)
                above = jnp.broadcast_to(halo_in[sweep, 0, at, :], plane)
                below = jnp.broadcast_to(halo_in[sweep, 1, at, :], plane)
                edge = jnp.where(row == 0, above, zero) + jnp.where(row == rows - 1, below, zero)
                of.append(coupling * edge)
            driven.append(of)
        turned = turn(q, driven)
        put(T, add(get(T, z), turned), z)
        return add(first, mul(get(PHI, z), turned)), add(last, mul(get(PSI, z), turned))


    loads[3].wait()
    for sweep in range(SWEEPS):

        sums = lax.fori_loop(0, depth, inner, (none, none))

        for piece in range(PIECES):
            for side in range(2):

                @pl.when(has["xy", side])
                def _():
                    halo_copy(sweep, side, piece).wait_recv()

            sums = lax.fori_loop(
                piece * zs, (piece + 1) * zs, functools.partial(outer, sweep), sums
            )
        put(ends, sums[0], 0)
        put(ends, sums[1], 1)


        if sweep == 0:
            near_side(pass_lam)
        near_side(functools.partial(own_sum, sweep))
        if sweep > 0:
            far_side(functools.partial(own_sum, sweep))
        near_side(functools.partial(pass_chain, sweep))
        if sweep == 0:
            far_side(pass_lam)
            far_side(functools.partial(own_sum, sweep))

        def forward(z, m):
            m = mul(get(PH, z), add(get(T, z), m))
            put(T, m, z)
            return m

        def backward(k, w):
            z = depth - 1 - k
            w = add(get(T, z), mul(get(PH, z), w))
            put(T, w, z)
            return w


        lax.fori_loop(0, depth, forward, none)
        lax.fori_loop(0, depth, backward, none)

        if sweep == 0:
            for side in range(2):
                lam = get(coef, 10 + side)
                away = tuple(
                    jnp.stack([lam_out[1 - side, j, p] for j in range(3)]) for p in range(2)
                )
                det = inv(one_minus(mul(lam, away)))
                put(coef, det, 6 + side)
                put(coef, mul(det, lam), 4 + side)
        far_side(functools.partial(pass_chain, sweep))


        for side in range(2):
            for j in range(3):
                arrived = (value_in[side, j, 0], value_in[side, j, 1])
                other = (ch_out[sweep, 1 - side, j, 0], ch_out[sweep, 1 - side, j, 1])
                value = add(
                    mul((coef[6 + side, 0, j], coef[6 + side, 1, j]), arrived),
                    mul((coef[4 + side, 0, j], coef[4 + side, 1, j]), other),
                )
                near[side, 0, j] = value[0]
                near[side, 1, j] = value[1]

        final = sweep == SWEEPS - 1

        def join(z, carry):
            q = matrix()
            before, after = get(near, 0), get(near, 1)
            w = add(add(get(T, z), mul(get(PHI, z), before)), mul(get(PSI, z), after))
            values = []
            for p in range(2):
                for c in range(3):
                    values.append(q[c][0] * w[p][0] + q[c][1] * w[p][1] + q[c][2] * w[p][2])
            target = OUT if final else U
            for i in range(6):
                target[z, i // 3, i % 3] = values[i]
            if not final:
                pack(sweep + 1, z, values)
            return carry


        for piece in range(PIECES):
            lax.fori_loop(piece * zs, (piece + 1) * zs, join, 0)
            if final:
                span = pl.ds(piece * zs, zs)
                pltpu.make_async_copy(OUT.at[span], out.at[span], out_sems.at[piece]).start()
            else:
                send_halo(sweep + 1, piece)


    for side in range(2):

        @pl.when(has["xy", 1 - side])
        def _():
            for sweep in range(SWEEPS):
                for piece in range(PIECES):
                    halo_copy(sweep, side, piece).wait_send()

        sends = both(even[side], onward[side] >= 1)

        @pl.when(sends)
        def _():
            for j in range(3):
                info_copy(side, j).wait_send()
                for sweep in range(SWEEPS):
                    own_copy(sweep, side, j).wait_send()

        @pl.when(both(sends, place[side] > 0))
        def _():
            for j in range(3, 9):
                info_copy(side, j).wait_send()

        for steps in (2, 1):

            @pl.when(both(odd[side], onward[side] >= steps))
            def _():
                for j in range(3):
                    lam_copy(side, steps, j).wait_send()
                    for sweep in range(SWEEPS):
                        x_copy(sweep, side, steps, j).wait_send()

    for piece in range(PIECES):
        span = pl.ds(piece * zs, zs)
        pltpu.make_async_copy(OUT.at[span], out.at[span], out_sems.at[piece]).wait()


def local(ngz, nxy, field, source, classes, boundary, conductance, angles, strengths):
    depth, _, _, rows, width = field.shape
    f32 = jnp.float32
    block = pltpu.VMEM(field.shape, f32)
    flat = (depth, rows, width)
    line = (2, 3, rows, width)
    pair = (2, rows, width)
    dma = pltpu.SemaphoreType.DMA
    hbm = pl.BlockSpec(memory_space=pl.ANY)
    smem = pl.BlockSpec(memory_space=pltpu.SMEM)
    return pl.pallas_call(
        functools.partial(relax, ngz, nxy),
        out_shape=jax.ShapeDtypeStruct(field.shape, f32),
        in_specs=[hbm] * 4 + [smem] * 3,
        out_specs=hbm,
        scratch_shapes=[
            block,
            block,
            pltpu.VMEM(flat, jnp.int32),
            pltpu.VMEM(flat, jnp.int32),
            pltpu.VMEM(flat, f32),
            pltpu.VMEM(flat, f32),
            block,
            block,
            block,
            block,
            block,
            pltpu.VMEM((3, 3, rows, 128), f32),
            pltpu.VMEM((2,) + line, f32),
            pltpu.VMEM((12,) + line, f32),
            pltpu.VMEM((2,) + line, f32),
            pltpu.VMEM((SWEEPS, 2, depth * 6, width), f32),
            pltpu.VMEM((SWEEPS, 2, depth * 6, width), f32),
            pltpu.VMEM((2, 3) + pair, f32),
            pltpu.VMEM((2, 9) + pair, f32),
            pltpu.VMEM((2, 9) + pair, f32),
            pltpu.VMEM((2, 3) + pair, f32),
            pltpu.VMEM((2, 3) + pair, f32),
            pltpu.VMEM((SWEEPS, 2, 3) + pair, f32),
            pltpu.VMEM((SWEEPS, 2, 3) + pair, f32),
            pltpu.VMEM((SWEEPS, 2, 3) + pair, f32),
            pltpu.VMEM((SWEEPS, 2, 3) + pair, f32),
            dma((4,)),
            dma((PIECES,)),
            dma((SWEEPS, 2, PIECES)),
            dma((SWEEPS, 2, PIECES)),
            dma((2, 9)),
            dma((2, 9)),
            dma((2, 2, 3)),
            dma((2, 3)),
            dma((SWEEPS, 2, 3)),
            dma((SWEEPS, 2, 3)),
            dma((SWEEPS, 2, 2, 3)),
            dma((SWEEPS, 2, 3)),
        ],
        compiler_params=pltpu.CompilerParams(collective_id=0, has_side_effects=True),
    )(field, source, classes, boundary, conductance, angles, strengths)


def solution(mesh):
    in_specs = (
        P("gz", None, None, "xy", None),
        P("gz", None, None, "xy", None),
        P("gz", "xy", None),
        P("gz", "xy", None),
        P(),
        P(),
        P(),
    )
    out_specs = P("gz", None, None, "xy", None)
    body = functools.partial(local, mesh.shape["gz"], mesh.shape["xy"])
    return jax.shard_map(body, mesh=mesh, in_specs=in_specs, out_specs=out_specs, check_vma=False)
```

```python
import functools

import jax
import jax.numpy as jnp
from jax import lax
from jax.experimental import pallas as pl
from jax.experimental.pallas import tpu as pltpu
from jax.sharding import PartitionSpec as P

SWEEPS = 2
PIECES = 2

coupling = 0.1
penalty = 4.0


def mul(a, b):
    return (a[0] * b[0] - a[1] * b[1], a[0] * b[1] + a[1] * b[0])


def add(a, b):
    return (a[0] + b[0], a[1] + b[1])


def inv(a):
    weight = 1.0 / (a[0] * a[0] + a[1] * a[1])
    return (a[0] * weight, -a[1] * weight)


def one_minus(a):
    return (1.0 - a[0], -a[1])


def get(ref, *at):
    return (ref[at + (0,)], ref[at + (1,)])


def put(ref, value, *at):
    ref[at + (0,)] = value[0]
    ref[at + (1,)] = value[1]


def loop(low, high, body, carry, by):
    by = by if (high - low) % by == 0 else 1

    def several(k, carry):
        for i in range(by):
            carry = body(low + k * by + i, carry)
        return carry

    return lax.fori_loop(0, (high - low) // by, several, carry)


def rotation(angles, shape):
    cos = [jnp.cos(jnp.full(shape, angles[i], jnp.float32)) for i in range(3)]
    sin = [jnp.sin(jnp.full(shape, angles[i], jnp.float32)) for i in range(3)]
    (ca, cb, cc), (sa, sb, sc) = cos, sin
    left = [[ca * cb, -sa, ca * sb], [sa * cb, ca, sa * sb], [-sb, jnp.zeros_like(cb), cb]]
    return [[row[0] * cc + row[1] * sc, row[1] * cc - row[0] * sc, row[2]] for row in left]


def relax(
    ngz,
    nxy,
    field,
    source,
    classes,
    boundary,
    conductance,
    angles,
    strengths,
    out,
    U,
    S,
    C,
    B,
    SG,
    DR,
    PH,
    PHI,
    PSI,
    T,
    OUT,
    QM,
    ends,
    coef,
    near,
    halo_out,
    halo_in,
    value_in,
    info_in,
    info_out,
    lam_in,
    lam_out,
    extra_in,
    extra_out,
    own_in,
    own_out,
    ch_in,
    ch_out,
    in_sems,
    out_sems,
    halo_send,
    halo_recv,
    info_send,
    info_recv,
    lam_send,
    lam_recv,
    extra_send,
    extra_recv,
    own_send,
    own_recv,
    ch_send,
    ch_recv,
):
    ix, iz = lax.axis_index("xy"), lax.axis_index("gz")
    depth, _, _, rows, width = U.shape
    kinds = conductance.shape[0]
    plane = (rows, width)
    has = {
        ("xy", 0): ix > 0,
        ("xy", 1): ix < nxy - 1,
    }
    where_is = {
        ("xy", 0): ix - 1,
        ("xy", 1): ix + 1,
    }
    for steps in (1, 2):
        has["gz", -steps] = iz >= steps
        has["gz", steps] = iz < ngz - steps
        where_is["gz", -steps] = iz - steps
        where_is["gz", steps] = iz + steps
    loads = [
        pltpu.make_async_copy(src, dst, in_sems.at[i])
        for i, (src, dst) in enumerate(((field, U), (classes, C), (boundary, B), (source, S)))
    ]
    for load in loads:
        load.start()

    barrier = pltpu.get_barrier_semaphore()
    for key, there in has.items():

        @pl.when(there)
        def _():
            pl.semaphore_signal(
                barrier,
                inc=1,
                device_id={key[0]: where_is[key]},
                device_id_type=pl.DeviceIdType.MESH,
            )


    def remote(src, dst, send, recv, key):
        return pltpu.make_async_remote_copy(
            src_ref=src,
            dst_ref=dst,
            send_sem=send,
            recv_sem=recv,
            device_id={key[0]: where_is[key]},
            device_id_type=pl.DeviceIdType.MESH,
        )

    zs = depth // PIECES
    lines = zs * 6

    def halo_copy(sweep, side, piece):
        span = pl.ds(piece * lines, lines)
        return remote(
            halo_out.at[sweep, side, span],
            halo_in.at[sweep, side, span],
            halo_send.at[sweep, side, piece],
            halo_recv.at[sweep, side, piece],
            ("xy", 1 - side),
        )

    def send_halo(sweep, piece):
        for side in range(2):

            @pl.when(has["xy", 1 - side])
            def _():
                halo_copy(sweep, side, piece).start()

    def pack(sweep, z, values):
        for i in range(6):
            halo_out[sweep, 0, pl.ds(z * 6 + i, 1), :] = values[i][rows - 1 :, :]
            halo_out[sweep, 1, pl.ds(z * 6 + i, 1), :] = values[i][:1, :]

    for side in range(2):

        @pl.when(jnp.logical_not(has["xy", side]))
        def _():
            for sweep in range(SWEEPS):
                halo_in[sweep, side] = jnp.zeros(halo_in.shape[2:], jnp.float32)

        @pl.when((iz if side == 0 else ngz - 1 - iz) < 2)
        def _():
            for part in range(3, 9):
                info_in[side, part] = jnp.zeros(info_in.shape[2:], jnp.float32)
            extra_in[side] = jnp.zeros(extra_in.shape[1:], jnp.float32)
            lam_in[side] = jnp.zeros(lam_in.shape[1:], jnp.float32)
            for sweep in range(SWEEPS):
                for j in range(3):
                    ch_in[sweep, side, j] = jnp.zeros(ch_in.shape[3:], jnp.float32)

    loads[0].wait()

    def pack_first(z, carry):
        pack(0, z, [U[z, i // 3, i % 3] for i in range(6)])
        return carry

    loop(0, depth, pack_first, 0, 4)
    count = sum(there.astype(jnp.int32) for there in has.values())
    pl.semaphore_wait(barrier, count)
    for piece in range(PIECES):
        send_halo(0, piece)

    loads[1].wait()
    loads[2].wait()

    def diagonal(z, carry):
        ids = C[z]
        sigma = jnp.zeros(plane, jnp.float32)
        for kind in range(kinds):
            sigma = jnp.where(ids == kind, conductance[kind], sigma)
        SG[z] = sigma
        DR[z] = 2.0 + 4.0 * coupling + penalty * B[z].astype(jnp.float32)
        return carry

    loop(0, depth, diagonal, 0, 4)

    def diag(z):
        real = jnp.broadcast_to(DR[z][None], (3,) + plane)
        sigma = SG[z]
        return real, jnp.stack([sigma * strengths[j] for j in range(3)])

    none = (jnp.zeros((3,) + plane, jnp.float32),) * 2

    def pivots(k, carry):
        p, q = carry
        z, back = k, depth - 1 - k
        d, f = diag(z), diag(back)
        p = inv((d[0] - p[0], d[1] - p[1]))
        q = inv((f[0] - q[0], f[1] - q[1]))
        put(PH, p, z)
        put(PHI, q, back)
        return p, q

    loop(0, depth, pivots, (none, none), 2)
    ones = (jnp.ones((3,) + plane, jnp.float32), none[0])

    def columns(k, carry):
        down, up = carry
        z, back = k, depth - 1 - k
        down = mul(get(PHI, z), down)
        up = mul(get(PH, back), up)
        put(PHI, down, z)
        put(PSI, up, back)
        return down, up

    loop(0, depth, columns, (ones, ones), 2)
    LEFT, RIGHT = 0, 1
    tip = (lambda: get(PHI, 0), lambda: get(PSI, depth - 1))
    across = lambda: get(PSI, 0)

    place = (iz, ngz - 1 - iz)
    even = [lax.rem(k, 2) == 0 for k in place]
    odd = [lax.rem(k, 2) == 1 for k in place]
    onward = [ngz - 1 - k for k in place]

    def to(side, steps):
        return {"gz": iz + steps if side == LEFT else iz - steps}

    def chain_copy(src, dst, send, recv, side, steps):
        return pltpu.make_async_remote_copy(
            src_ref=src,
            dst_ref=dst,
            send_sem=send,
            recv_sem=recv,
            device_id=to(side, steps),
            device_id_type=pl.DeviceIdType.MESH,
        )

    def info_copy(side, j):
        return chain_copy(
            info_out.at[side, j],
            info_in.at[side, j],
            info_send.at[side, j],
            info_recv.at[side, j],
            side,
            1,
        )

    def lam_copy(side, steps, j):
        return chain_copy(
            lam_out.at[side, j],
            lam_in.at[side, j],
            lam_send.at[side, steps - 1, j],
            lam_recv.at[side, j],
            side,
            steps,
        )

    def own_copy(sweep, side, j):
        return chain_copy(
            own_out.at[sweep, side, j],
            own_in.at[sweep, side, j],
            own_send.at[sweep, side, j],
            own_recv.at[sweep, side, j],
            side,
            1,
        )

    def x_copy(sweep, side, steps, j):
        return chain_copy(
            ch_out.at[sweep, side, j],
            ch_in.at[sweep, side, j],
            ch_send.at[sweep, side, steps - 1, j],
            ch_recv.at[sweep, side, j],
            side,
            steps,
        )

    both = jnp.logical_and

    def send_info(side):
        parts = (tip[1 - side](), tip[side](), across())
        for part in range(3):
            for j in range(3):
                for p in range(2):
                    info_out[side, part * 3 + j, p] = parts[part][p][j]
            sends = both(even[side], onward[side] >= 1)

            @pl.when(sends if part == 0 else both(sends, place[side] > 0))
            def _():
                for j in range(3):
                    info_copy(side, part * 3 + j).start()

    def pass_lam(side):
        @pl.when(odd[side])
        def _():
            for j in range(3):
                info_copy(side, j).wait_recv()

        @pl.when(both(odd[side], place[side] >= 2))
        def _():
            for j in range(3, 9):
                info_copy(side, j).wait_recv()

        @pl.when(place[side] >= 2)
        def _():
            for j in range(3):
                lam_copy(side, 1, j).wait_recv()

        for j in range(3):
            tips = [(info_in[side, 3 * k + j, 0], info_in[side, 3 * k + j, 1]) for k in range(3)]
            given = (lam_in[side, j, 0], lam_in[side, j, 1])

            @pl.when(odd[side])
            def _():
                skip = mul(tips[2], inv(one_minus(mul(tips[1], given))))
                along = mul(skip, given)
                lam = add(tips[0], mul(tips[2], along))
                for p in range(2):
                    coef[12 + side, p, j] = along[p]
                    coef[8 + side, p, j] = skip[p]
                    coef[10 + side, p, j] = lam[p]

            @pl.when(even[side])
            def _():
                for p in range(2):
                    coef[10 + side, p, j] = given[p]

            of = lambda pair: (pair[0][j], pair[1][j])
            lam = (coef[10 + side, 0, j], coef[10 + side, 1, j])
            kappa = mul(of(across()), inv(one_minus(mul(of(tip[side]()), lam))))
            over = mul(kappa, lam)
            value = add(of(tip[1 - side]()), mul(of(across()), over))
            for p in range(2):
                coef[side, p, j] = kappa[p]
                coef[2 + side, p, j] = over[p]
                lam_out[side, j, p] = value[p]

            for steps in (2, 1):

                @pl.when(both(odd[side], onward[side] >= steps))
                def _():
                    lam_copy(side, steps, j).start()

    def extra_copy(side, j):
        return chain_copy(
            extra_out.at[side, j],
            extra_in.at[side, j],
            extra_send.at[side, j],
            extra_recv.at[side, j],
            side,
            1,
        )

    def own_base(side, j):
        return add(
            (ends[1 - side, 0, j], ends[1 - side, 1, j]),
            mul(
                (coef[2 + side, 0, j], coef[2 + side, 1, j]),
                (ends[side, 0, j], ends[side, 1, j]),
            ),
        )

    def own_sum(sweep, side):
        for j in range(3):
            if sweep == 0:
                for p in range(2):
                    own_out[sweep, side, j, p] = ends[1 - side, p, j]
                    extra_out[side, j, p] = ends[side, p, j]
            else:
                base = own_base(side, j)
                for p in range(2):
                    own_out[sweep, side, j, p] = base[p]
            sends = both(even[side], onward[side] >= 1)

            @pl.when(sends)
            def _():
                own_copy(sweep, side, j).start()

            if sweep == 0:

                @pl.when(both(sends, place[side] > 0))
                def _():
                    extra_copy(side, j).start()

    def pass_chain(sweep, side):
        for j in range(3):
            base = own_base(side, j)

            @pl.when(odd[side])
            def _():
                own_copy(sweep, side, j).wait_recv()

            if sweep == 0:

                @pl.when(both(odd[side], place[side] >= 2))
                def _():
                    extra_copy(side, j).wait_recv()

            @pl.when(place[side] >= 2)
            def _():
                x_copy(sweep, side, 1, j).wait_recv()

            given = (ch_in[sweep, side, j, 0], ch_in[sweep, side, j, 1])

            @pl.when(odd[side])
            def _():
                own = (own_in[sweep, side, j, 0], own_in[sweep, side, j, 1])
                if sweep == 0:
                    extra = (extra_in[side, j, 0], extra_in[side, j, 1])
                    own = add(own, mul((coef[12 + side, 0, j], coef[12 + side, 1, j]), extra))
                x = add(own, mul((coef[8 + side, 0, j], coef[8 + side, 1, j]), given))
                for p in range(2):
                    value_in[side, j, p] = x[p]

            @pl.when(even[side])
            def _():
                for p in range(2):
                    value_in[side, j, p] = given[p]

            x = (value_in[side, j, 0], value_in[side, j, 1])
            result = add(base, mul((coef[side, 0, j], coef[side, 1, j]), x))
            for p in range(2):
                ch_out[sweep, side, j, p] = result[p]

            for steps in (2, 1):

                @pl.when(both(odd[side], onward[side] >= steps))
                def _():
                    x_copy(sweep, side, steps, j).start()

    left_first = iz * 2 < ngz - 1

    def near_side(run):
        @pl.when(left_first)
        def _():
            run(LEFT)

        @pl.when(jnp.logical_not(left_first))
        def _():
            run(RIGHT)

    def far_side(run):
        @pl.when(left_first)
        def _():
            run(RIGHT)

        @pl.when(jnp.logical_not(left_first))
        def _():
            run(LEFT)

    near_side(send_info)
    far_side(send_info)

    angle_matrix = rotation(angles, (rows, 128))
    for c in range(3):
        for j in range(3):
            QM[c, j] = angle_matrix[c][j]

    def matrix():
        return [
            [jnp.concatenate([QM[c, j]] * (width // 128), axis=1) for j in range(3)]
            for c in range(3)
        ]

    row = lax.broadcasted_iota(jnp.int32, plane, 0)
    lane = lax.broadcasted_iota(jnp.int32, plane, 1)
    zero = jnp.zeros(plane, jnp.float32)

    def turn(q, driven):
        return [
            jnp.stack(
                [
                    q[0][j] * driven[p][0] + q[1][j] * driven[p][1] + q[2][j] * driven[p][2]
                    for j in range(3)
                ]
            )
            for p in range(2)
        ]

    def inner(z, carry):
        first, last = carry
        q = matrix()
        driven = []
        for p in range(2):
            of = []
            for c in range(3):
                u = U[z, p, c]
                beside = jnp.where(lane == 0, zero, pltpu.roll(u, 1, 1))
                beside += jnp.where(lane == width - 1, zero, pltpu.roll(u, width - 1, 1))
                beside += jnp.where(row == 0, zero, pltpu.roll(u, 1, 0))
                beside += jnp.where(row == rows - 1, zero, pltpu.roll(u, rows - 1, 0))
                of.append(S[z, p, c] + coupling * beside)
            driven.append(of)
        turned = turn(q, driven)
        put(T, turned, z)
        return add(first, mul(get(PHI, z), turned)), add(last, mul(get(PSI, z), turned))

    def outer(sweep, z, carry):
        first, last = carry
        q = matrix()
        driven = []
        for p in range(2):
            of = []
            for c in range(3):
                at = pl.ds(z * 6 + p * 3 + c, 1)
                above = jnp.broadcast_to(halo_in[sweep, 0, at, :], plane)
                below = jnp.broadcast_to(halo_in[sweep, 1, at, :], plane)
                edge = jnp.where(row == 0, above, zero) + jnp.where(row == rows - 1, below, zero)
                of.append(coupling * edge)
            driven.append(of)
        turned = turn(q, driven)
        put(T, add(get(T, z), turned), z)
        return add(first, mul(get(PHI, z), turned)), add(last, mul(get(PSI, z), turned))

    loads[3].wait()
    for sweep in range(SWEEPS):
        sums = loop(0, depth, inner, (none, none), 4)
        for piece in range(PIECES):
            for side in range(2):

                @pl.when(has["xy", side])
                def _():
                    halo_copy(sweep, side, piece).wait_recv()

            sums = loop(
                piece * zs, (piece + 1) * zs, functools.partial(outer, sweep), sums, 4
            )
        put(ends, sums[0], 0)
        put(ends, sums[1], 1)

        near_side(functools.partial(own_sum, sweep))
        far_side(functools.partial(own_sum, sweep))
        if sweep == 0:
            near_side(pass_lam)
        near_side(functools.partial(pass_chain, sweep))

        def forward(z, m):
            m = mul(get(PH, z), add(get(T, z), m))
            put(T, m, z)
            return m

        def backward(k, w):
            z = depth - 1 - k
            w = add(get(T, z), mul(get(PH, z), w))
            put(T, w, z)
            return w

        loop(0, depth, forward, none, 4)
        loop(0, depth, backward, none, 4)
        if sweep == 0:
            far_side(pass_lam)
            for side in range(2):
                lam = get(coef, 10 + side)
                away = tuple(
                    jnp.stack([lam_out[1 - side, j, p] for j in range(3)]) for p in range(2)
                )
                det = inv(one_minus(mul(lam, away)))
                put(coef, det, 6 + side)
                put(coef, mul(det, lam), 4 + side)
        far_side(functools.partial(pass_chain, sweep))

        for side in range(2):
            for j in range(3):
                arrived = (value_in[side, j, 0], value_in[side, j, 1])
                other = (ch_out[sweep, 1 - side, j, 0], ch_out[sweep, 1 - side, j, 1])
                value = add(
                    mul((coef[6 + side, 0, j], coef[6 + side, 1, j]), arrived),
                    mul((coef[4 + side, 0, j], coef[4 + side, 1, j]), other),
                )
                near[side, 0, j] = value[0]
                near[side, 1, j] = value[1]

        final = sweep == SWEEPS - 1

        def join(z, carry):
            q = matrix()
            before, after = get(near, 0), get(near, 1)
            w = add(add(get(T, z), mul(get(PHI, z), before)), mul(get(PSI, z), after))
            values = []
            for p in range(2):
                for c in range(3):
                    values.append(q[c][0] * w[p][0] + q[c][1] * w[p][1] + q[c][2] * w[p][2])
            target = OUT if final else U
            for i in range(6):
                target[z, i // 3, i % 3] = values[i]
            if not final:
                pack(sweep + 1, z, values)
            return carry

        for piece in range(PIECES):
            loop(piece * zs, (piece + 1) * zs, join, 0, 4)
            if final:
                span = pl.ds(piece * zs, zs)
                pltpu.make_async_copy(OUT.at[span], out.at[span], out_sems.at[piece]).start()
            else:
                send_halo(sweep + 1, piece)

    for side in range(2):

        @pl.when(has["xy", 1 - side])
        def _():
            for sweep in range(SWEEPS):
                for piece in range(PIECES):
                    halo_copy(sweep, side, piece).wait_send()

        sends = both(even[side], onward[side] >= 1)

        @pl.when(sends)
        def _():
            for j in range(3):
                info_copy(side, j).wait_send()
                for sweep in range(SWEEPS):
                    own_copy(sweep, side, j).wait_send()

        @pl.when(both(sends, place[side] > 0))
        def _():
            for j in range(3, 9):
                info_copy(side, j).wait_send()
            for j in range(3):
                extra_copy(side, j).wait_send()

        for steps in (2, 1):

            @pl.when(both(odd[side], onward[side] >= steps))
            def _():
                for j in range(3):
                    lam_copy(side, steps, j).wait_send()
                    for sweep in range(SWEEPS):
                        x_copy(sweep, side, steps, j).wait_send()

    for piece in range(PIECES):
        span = pl.ds(piece * zs, zs)
        pltpu.make_async_copy(OUT.at[span], out.at[span], out_sems.at[piece]).wait()


def local(ngz, nxy, field, source, classes, boundary, conductance, angles, strengths):
    depth, _, _, rows, width = field.shape
    f32 = jnp.float32
    block = pltpu.VMEM(field.shape, f32)
    flat = (depth, rows, width)
    line = (2, 3, rows, width)
    pair = (2, rows, width)
    dma = pltpu.SemaphoreType.DMA
    hbm = pl.BlockSpec(memory_space=pl.ANY)
    smem = pl.BlockSpec(memory_space=pltpu.SMEM)
    return pl.pallas_call(
        functools.partial(relax, ngz, nxy),
        out_shape=jax.ShapeDtypeStruct(field.shape, f32),
        in_specs=[hbm] * 4 + [smem] * 3,
        out_specs=hbm,
        scratch_shapes=[
            block,
            block,
            pltpu.VMEM(flat, jnp.int32),
            pltpu.VMEM(flat, jnp.int32),
            pltpu.VMEM(flat, f32),
            pltpu.VMEM(flat, f32),
            block,
            block,
            block,
            block,
            block,
            pltpu.VMEM((3, 3, rows, 128), f32),
            pltpu.VMEM((2,) + line, f32),
            pltpu.VMEM((14,) + line, f32),
            pltpu.VMEM((2,) + line, f32),
            pltpu.VMEM((SWEEPS, 2, depth * 6, width), f32),
            pltpu.VMEM((SWEEPS, 2, depth * 6, width), f32),
            pltpu.VMEM((2, 3) + pair, f32),
            pltpu.VMEM((2, 9) + pair, f32),
            pltpu.VMEM((2, 9) + pair, f32),
            pltpu.VMEM((2, 3) + pair, f32),
            pltpu.VMEM((2, 3) + pair, f32),
            pltpu.VMEM((2, 3) + pair, f32),
            pltpu.VMEM((2, 3) + pair, f32),
            pltpu.VMEM((SWEEPS, 2, 3) + pair, f32),
            pltpu.VMEM((SWEEPS, 2, 3) + pair, f32),
            pltpu.VMEM((SWEEPS, 2, 3) + pair, f32),
            pltpu.VMEM((SWEEPS, 2, 3) + pair, f32),
            dma((4,)),
            dma((PIECES,)),
            dma((SWEEPS, 2, PIECES)),
            dma((SWEEPS, 2, PIECES)),
            dma((2, 9)),
            dma((2, 9)),
            dma((2, 2, 3)),
            dma((2, 3)),
            dma((2, 3)),
            dma((2, 3)),
            dma((SWEEPS, 2, 3)),
            dma((SWEEPS, 2, 3)),
            dma((SWEEPS, 2, 2, 3)),
            dma((SWEEPS, 2, 3)),
        ],
        compiler_params=pltpu.CompilerParams(collective_id=0, has_side_effects=True),
    )(field, source, classes, boundary, conductance, angles, strengths)


def solution(mesh):
    in_specs = (
        P("gz", None, None, "xy", None),
        P("gz", None, None, "xy", None),
        P("gz", "xy", None),
        P("gz", "xy", None),
        P(),
        P(),
        P(),
    )
    out_specs = P("gz", None, None, "xy", None)
    body = functools.partial(local, mesh.shape["gz"], mesh.shape["xy"])
    return jax.shard_map(body, mesh=mesh, in_specs=in_specs, out_specs=out_specs, check_vma=False)
```

```python
import functools

import jax
import jax.numpy as jnp
from jax import lax
from jax.experimental import pallas as pl
from jax.experimental.pallas import tpu as pltpu
from jax.sharding import PartitionSpec as P

SWEEPS = 2
PIECES = 2
VMEM_LIMIT = 62 * 2**20

coupling = 0.1
penalty = 4.0


def mul(a, b):
    return (a[0] * b[0] - a[1] * b[1], a[0] * b[1] + a[1] * b[0])


def add(a, b):
    return (a[0] + b[0], a[1] + b[1])


def inv(a):
    weight = 1.0 / (a[0] * a[0] + a[1] * a[1])
    return (a[0] * weight, -a[1] * weight)


def one_minus(a):
    return (1.0 - a[0], -a[1])


def get(ref, *at):
    return (ref[at + (0,)], ref[at + (1,)])


def put(ref, value, *at):
    ref[at + (0,)] = value[0]
    ref[at + (1,)] = value[1]


def loop(low, high, body, carry, by):
    by = by if (high - low) % by == 0 else 1

    def several(k, carry):
        for i in range(by):
            carry = body(low + k * by + i, carry)
        return carry

    return lax.fori_loop(0, (high - low) // by, several, carry)


def rotation(angles, shape):
    cos = [jnp.cos(jnp.full(shape, angles[i], jnp.float32)) for i in range(3)]
    sin = [jnp.sin(jnp.full(shape, angles[i], jnp.float32)) for i in range(3)]
    (ca, cb, cc), (sa, sb, sc) = cos, sin
    left = [[ca * cb, -sa, ca * sb], [sa * cb, ca, sa * sb], [-sb, jnp.zeros_like(cb), cb]]
    return [[row[0] * cc + row[1] * sc, row[1] * cc - row[0] * sc, row[2]] for row in left]


def relax(
    ngz,
    nxy,
    field,
    source,
    classes,
    boundary,
    conductance,
    angles,
    strengths,
    OUT,
    U,
    S,
    C,
    B,
    SG,
    DR,
    PH,
    PHI,
    PSI,
    T,
    QM,
    ends,
    coef,
    near,
    halo_out,
    halo_in,
    value_in,
    info_in,
    info_out,
    lam_in,
    lam_out,
    extra_in,
    extra_out,
    own_in,
    own_out,
    ch_in,
    ch_out,
    in_sems,
    halo_send,
    halo_recv,
    info_send,
    info_recv,
    lam_send,
    lam_recv,
    extra_send,
    extra_recv,
    own_send,
    own_recv,
    ch_send,
    ch_recv,
):
    ix, iz = lax.axis_index("xy"), lax.axis_index("gz")
    depth, _, _, rows, width = U.shape
    kinds = conductance.shape[0]
    plane = (rows, width)
    has = {
        ("xy", 0): ix > 0,
        ("xy", 1): ix < nxy - 1,
    }
    where_is = {
        ("xy", 0): ix - 1,
        ("xy", 1): ix + 1,
    }
    for steps in (1, 2):
        has["gz", -steps] = iz >= steps
        has["gz", steps] = iz < ngz - steps
        where_is["gz", -steps] = iz - steps
        where_is["gz", steps] = iz + steps
    loads = [
        pltpu.make_async_copy(src, dst, in_sems.at[i])
        for i, (src, dst) in enumerate(((field, U), (classes, C), (boundary, B), (source, S)))
    ]
    for load in loads:
        load.start()

    barrier = pltpu.get_barrier_semaphore()
    for key, there in has.items():

        @pl.when(there)
        def _():
            pl.semaphore_signal(
                barrier,
                inc=1,
                device_id={key[0]: where_is[key]},
                device_id_type=pl.DeviceIdType.MESH,
            )


    def remote(src, dst, send, recv, key):
        return pltpu.make_async_remote_copy(
            src_ref=src,
            dst_ref=dst,
            send_sem=send,
            recv_sem=recv,
            device_id={key[0]: where_is[key]},
            device_id_type=pl.DeviceIdType.MESH,
        )

    zs = depth // PIECES
    lines = zs * 6

    def halo_copy(sweep, side, piece):
        span = pl.ds(piece * lines, lines)
        return remote(
            halo_out.at[sweep, side, span],
            halo_in.at[sweep, side, span],
            halo_send.at[sweep, side, piece],
            halo_recv.at[sweep, side, piece],
            ("xy", 1 - side),
        )

    def send_halo(sweep, piece):
        for side in range(2):

            @pl.when(has["xy", 1 - side])
            def _():
                halo_copy(sweep, side, piece).start()

    def pack(sweep, z, values):
        for i in range(6):
            halo_out[sweep, 0, pl.ds(z * 6 + i, 1), :] = values[i][rows - 1 :, :]
            halo_out[sweep, 1, pl.ds(z * 6 + i, 1), :] = values[i][:1, :]

    for side in range(2):

        @pl.when(jnp.logical_not(has["xy", side]))
        def _():
            for sweep in range(SWEEPS):
                halo_in[sweep, side] = jnp.zeros(halo_in.shape[2:], jnp.float32)

        @pl.when((iz if side == 0 else ngz - 1 - iz) < 2)
        def _():
            for part in range(3, 9):
                info_in[side, part] = jnp.zeros(info_in.shape[2:], jnp.float32)
            extra_in[side] = jnp.zeros(extra_in.shape[1:], jnp.float32)
            lam_in[side] = jnp.zeros(lam_in.shape[1:], jnp.float32)
            for sweep in range(SWEEPS):
                for j in range(3):
                    ch_in[sweep, side, j] = jnp.zeros(ch_in.shape[3:], jnp.float32)

    loads[0].wait()

    def pack_first(z, carry):
        pack(0, z, [U[z, i // 3, i % 3] for i in range(6)])
        return carry

    loop(0, depth, pack_first, 0, 4)
    count = sum(there.astype(jnp.int32) for there in has.values())
    pl.semaphore_wait(barrier, count)
    for piece in range(PIECES):
        send_halo(0, piece)

    loads[1].wait()
    loads[2].wait()

    def diagonal(z, carry):
        ids = C[z]
        sigma = jnp.zeros(plane, jnp.float32)
        for kind in range(kinds):
            sigma = jnp.where(ids == kind, conductance[kind], sigma)
        SG[z] = sigma
        DR[z] = 2.0 + 4.0 * coupling + penalty * B[z].astype(jnp.float32)
        return carry

    loop(0, depth, diagonal, 0, 4)

    def diag(z):
        real = jnp.broadcast_to(DR[z][None], (3,) + plane)
        sigma = SG[z]
        return real, jnp.stack([sigma * strengths[j] for j in range(3)])

    none = (jnp.zeros((3,) + plane, jnp.float32),) * 2

    def pivots(k, carry):
        p, q = carry
        z, back = k, depth - 1 - k
        d, f = diag(z), diag(back)
        p = inv((d[0] - p[0], d[1] - p[1]))
        q = inv((f[0] - q[0], f[1] - q[1]))
        put(PH, p, z)
        put(PHI, q, back)
        return p, q

    loop(0, depth, pivots, (none, none), 2)
    ones = (jnp.ones((3,) + plane, jnp.float32), none[0])

    def columns(k, carry):
        down, up = carry
        z, back = k, depth - 1 - k
        down = mul(get(PHI, z), down)
        up = mul(get(PH, back), up)
        put(PHI, down, z)
        put(PSI, up, back)
        return down, up

    loop(0, depth, columns, (ones, ones), 2)
    LEFT, RIGHT = 0, 1
    tip = (lambda: get(PHI, 0), lambda: get(PSI, depth - 1))
    across = lambda: get(PSI, 0)

    place = (iz, ngz - 1 - iz)
    even = [lax.rem(k, 2) == 0 for k in place]
    odd = [lax.rem(k, 2) == 1 for k in place]
    onward = [ngz - 1 - k for k in place]

    def to(side, steps):
        return {"gz": iz + steps if side == LEFT else iz - steps}

    def chain_copy(src, dst, send, recv, side, steps):
        return pltpu.make_async_remote_copy(
            src_ref=src,
            dst_ref=dst,
            send_sem=send,
            recv_sem=recv,
            device_id=to(side, steps),
            device_id_type=pl.DeviceIdType.MESH,
        )

    def info_copy(side, j):
        return chain_copy(
            info_out.at[side, j],
            info_in.at[side, j],
            info_send.at[side, j],
            info_recv.at[side, j],
            side,
            1,
        )

    def lam_copy(side, steps, j):
        return chain_copy(
            lam_out.at[side, j],
            lam_in.at[side, j],
            lam_send.at[side, steps - 1, j],
            lam_recv.at[side, j],
            side,
            steps,
        )

    def own_copy(sweep, side, j):
        return chain_copy(
            own_out.at[sweep, side, j],
            own_in.at[sweep, side, j],
            own_send.at[sweep, side, j],
            own_recv.at[sweep, side, j],
            side,
            1,
        )

    def x_copy(sweep, side, steps, j):
        return chain_copy(
            ch_out.at[sweep, side, j],
            ch_in.at[sweep, side, j],
            ch_send.at[sweep, side, steps - 1, j],
            ch_recv.at[sweep, side, j],
            side,
            steps,
        )

    both = jnp.logical_and

    def send_info(side):
        parts = (tip[1 - side](), tip[side](), across())
        for part in range(3):
            for j in range(3):
                for p in range(2):
                    info_out[side, part * 3 + j, p] = parts[part][p][j]
            sends = both(even[side], onward[side] >= 1)

            @pl.when(sends if part == 0 else both(sends, place[side] > 0))
            def _():
                for j in range(3):
                    info_copy(side, part * 3 + j).start()

    def pass_lam(side):
        @pl.when(odd[side])
        def _():
            for j in range(3):
                info_copy(side, j).wait_recv()

        @pl.when(both(odd[side], place[side] >= 2))
        def _():
            for j in range(3, 9):
                info_copy(side, j).wait_recv()

        @pl.when(place[side] >= 2)
        def _():
            for j in range(3):
                lam_copy(side, 1, j).wait_recv()

        for j in range(3):
            tips = [(info_in[side, 3 * k + j, 0], info_in[side, 3 * k + j, 1]) for k in range(3)]
            given = (lam_in[side, j, 0], lam_in[side, j, 1])

            @pl.when(odd[side])
            def _():
                skip = mul(tips[2], inv(one_minus(mul(tips[1], given))))
                along = mul(skip, given)
                lam = add(tips[0], mul(tips[2], along))
                for p in range(2):
                    coef[12 + side, p, j] = along[p]
                    coef[8 + side, p, j] = skip[p]
                    coef[10 + side, p, j] = lam[p]

            @pl.when(even[side])
            def _():
                for p in range(2):
                    coef[10 + side, p, j] = given[p]

            of = lambda pair: (pair[0][j], pair[1][j])
            lam = (coef[10 + side, 0, j], coef[10 + side, 1, j])
            kappa = mul(of(across()), inv(one_minus(mul(of(tip[side]()), lam))))
            over = mul(kappa, lam)
            value = add(of(tip[1 - side]()), mul(of(across()), over))
            for p in range(2):
                coef[side, p, j] = kappa[p]
                coef[2 + side, p, j] = over[p]
                lam_out[side, j, p] = value[p]

            for steps in (2, 1):

                @pl.when(both(odd[side], onward[side] >= steps))
                def _():
                    lam_copy(side, steps, j).start()

    def extra_copy(side, j):
        return chain_copy(
            extra_out.at[side, j],
            extra_in.at[side, j],
            extra_send.at[side, j],
            extra_recv.at[side, j],
            side,
            1,
        )

    def own_base(side, j):
        return add(
            (ends[1 - side, 0, j], ends[1 - side, 1, j]),
            mul(
                (coef[2 + side, 0, j], coef[2 + side, 1, j]),
                (ends[side, 0, j], ends[side, 1, j]),
            ),
        )

    def own_sum(sweep, side):
        for j in range(3):
            if sweep == 0:
                for p in range(2):
                    own_out[sweep, side, j, p] = ends[1 - side, p, j]
                    extra_out[side, j, p] = ends[side, p, j]
            else:
                base = own_base(side, j)
                for p in range(2):
                    own_out[sweep, side, j, p] = base[p]
            sends = both(even[side], onward[side] >= 1)

            @pl.when(sends)
            def _():
                own_copy(sweep, side, j).start()

            if sweep == 0:

                @pl.when(both(sends, place[side] > 0))
                def _():
                    extra_copy(side, j).start()

    def pass_chain(sweep, side):
        for j in range(3):
            base = own_base(side, j)

            @pl.when(odd[side])
            def _():
                own_copy(sweep, side, j).wait_recv()

            if sweep == 0:

                @pl.when(both(odd[side], place[side] >= 2))
                def _():
                    extra_copy(side, j).wait_recv()

            @pl.when(place[side] >= 2)
            def _():
                x_copy(sweep, side, 1, j).wait_recv()

            given = (ch_in[sweep, side, j, 0], ch_in[sweep, side, j, 1])

            @pl.when(odd[side])
            def _():
                own = (own_in[sweep, side, j, 0], own_in[sweep, side, j, 1])
                if sweep == 0:
                    extra = (extra_in[side, j, 0], extra_in[side, j, 1])
                    own = add(own, mul((coef[12 + side, 0, j], coef[12 + side, 1, j]), extra))
                x = add(own, mul((coef[8 + side, 0, j], coef[8 + side, 1, j]), given))
                for p in range(2):
                    value_in[side, j, p] = x[p]

            @pl.when(even[side])
            def _():
                for p in range(2):
                    value_in[side, j, p] = given[p]

            x = (value_in[side, j, 0], value_in[side, j, 1])
            result = add(base, mul((coef[side, 0, j], coef[side, 1, j]), x))
            for p in range(2):
                ch_out[sweep, side, j, p] = result[p]

            for steps in (2, 1):

                @pl.when(both(odd[side], onward[side] >= steps))
                def _():
                    x_copy(sweep, side, steps, j).start()

    left_first = iz * 2 < ngz - 1

    def near_side(run):
        @pl.when(left_first)
        def _():
            run(LEFT)

        @pl.when(jnp.logical_not(left_first))
        def _():
            run(RIGHT)

    def far_side(run):
        @pl.when(left_first)
        def _():
            run(RIGHT)

        @pl.when(jnp.logical_not(left_first))
        def _():
            run(LEFT)

    near_side(send_info)
    far_side(send_info)

    angle_matrix = rotation(angles, (rows, 128))
    for c in range(3):
        for j in range(3):
            QM[c, j] = angle_matrix[c][j]

    def matrix():
        return [
            [jnp.concatenate([QM[c, j]] * (width // 128), axis=1) for j in range(3)]
            for c in range(3)
        ]

    row = lax.broadcasted_iota(jnp.int32, plane, 0)
    lane = lax.broadcasted_iota(jnp.int32, plane, 1)
    zero = jnp.zeros(plane, jnp.float32)

    def turn(q, driven):
        return [
            jnp.stack(
                [
                    q[0][j] * driven[p][0] + q[1][j] * driven[p][1] + q[2][j] * driven[p][2]
                    for j in range(3)
                ]
            )
            for p in range(2)
        ]

    def inner(z, carry):
        first, last = carry
        q = matrix()
        driven = []
        for p in range(2):
            of = []
            for c in range(3):
                u = U[z, p, c]
                beside = jnp.where(lane == 0, zero, pltpu.roll(u, 1, 1))
                beside += jnp.where(lane == width - 1, zero, pltpu.roll(u, width - 1, 1))
                beside += jnp.where(row == 0, zero, pltpu.roll(u, 1, 0))
                beside += jnp.where(row == rows - 1, zero, pltpu.roll(u, rows - 1, 0))
                of.append(S[z, p, c] + coupling * beside)
            driven.append(of)
        turned = turn(q, driven)
        put(T, turned, z)
        return add(first, mul(get(PHI, z), turned)), add(last, mul(get(PSI, z), turned))

    def outer(sweep, z, carry):
        first, last = carry
        q = matrix()
        driven = []
        for p in range(2):
            of = []
            for c in range(3):
                at = pl.ds(z * 6 + p * 3 + c, 1)
                above = jnp.broadcast_to(halo_in[sweep, 0, at, :], plane)
                below = jnp.broadcast_to(halo_in[sweep, 1, at, :], plane)
                edge = jnp.where(row == 0, above, zero) + jnp.where(row == rows - 1, below, zero)
                of.append(coupling * edge)
            driven.append(of)
        turned = turn(q, driven)
        put(T, add(get(T, z), turned), z)
        return add(first, mul(get(PHI, z), turned)), add(last, mul(get(PSI, z), turned))

    loads[3].wait()
    for sweep in range(SWEEPS):
        sums = loop(0, depth, inner, (none, none), 4)
        for piece in range(PIECES):
            for side in range(2):

                @pl.when(has["xy", side])
                def _():
                    halo_copy(sweep, side, piece).wait_recv()

            sums = loop(
                piece * zs, (piece + 1) * zs, functools.partial(outer, sweep), sums, 4
            )
        put(ends, sums[0], 0)
        put(ends, sums[1], 1)

        near_side(functools.partial(own_sum, sweep))
        far_side(functools.partial(own_sum, sweep))
        if sweep == 0:
            near_side(pass_lam)
        near_side(functools.partial(pass_chain, sweep))

        def forward(z, m):
            m = mul(get(PH, z), add(get(T, z), m))
            put(T, m, z)
            return m

        def backward(k, w):
            z = depth - 1 - k
            w = add(get(T, z), mul(get(PH, z), w))
            put(T, w, z)
            return w

        loop(0, depth, forward, none, 4)
        loop(0, depth, backward, none, 4)
        if sweep == 0:
            far_side(pass_lam)
            for side in range(2):
                lam = get(coef, 10 + side)
                away = tuple(
                    jnp.stack([lam_out[1 - side, j, p] for j in range(3)]) for p in range(2)
                )
                det = inv(one_minus(mul(lam, away)))
                put(coef, det, 6 + side)
                put(coef, mul(det, lam), 4 + side)
        far_side(functools.partial(pass_chain, sweep))

        for side in range(2):
            for j in range(3):
                arrived = (value_in[side, j, 0], value_in[side, j, 1])
                other = (ch_out[sweep, 1 - side, j, 0], ch_out[sweep, 1 - side, j, 1])
                value = add(
                    mul((coef[6 + side, 0, j], coef[6 + side, 1, j]), arrived),
                    mul((coef[4 + side, 0, j], coef[4 + side, 1, j]), other),
                )
                near[side, 0, j] = value[0]
                near[side, 1, j] = value[1]

        final = sweep == SWEEPS - 1

        def join(z, carry):
            q = matrix()
            before, after = get(near, 0), get(near, 1)
            w = add(add(get(T, z), mul(get(PHI, z), before)), mul(get(PSI, z), after))
            values = []
            for p in range(2):
                for c in range(3):
                    values.append(q[c][0] * w[p][0] + q[c][1] * w[p][1] + q[c][2] * w[p][2])
            target = OUT if final else U
            for i in range(6):
                target[z, i // 3, i % 3] = values[i]
            if not final:
                pack(sweep + 1, z, values)
            return carry

        for piece in range(PIECES):
            loop(piece * zs, (piece + 1) * zs, join, 0, 4)
            if not final:
                send_halo(sweep + 1, piece)

    for side in range(2):

        @pl.when(has["xy", 1 - side])
        def _():
            for sweep in range(SWEEPS):
                for piece in range(PIECES):
                    halo_copy(sweep, side, piece).wait_send()

        sends = both(even[side], onward[side] >= 1)

        @pl.when(sends)
        def _():
            for j in range(3):
                info_copy(side, j).wait_send()
                for sweep in range(SWEEPS):
                    own_copy(sweep, side, j).wait_send()

        @pl.when(both(sends, place[side] > 0))
        def _():
            for j in range(3, 9):
                info_copy(side, j).wait_send()
            for j in range(3):
                extra_copy(side, j).wait_send()

        for steps in (2, 1):

            @pl.when(both(odd[side], onward[side] >= steps))
            def _():
                for j in range(3):
                    lam_copy(side, steps, j).wait_send()
                    for sweep in range(SWEEPS):
                        x_copy(sweep, side, steps, j).wait_send()


def local(ngz, nxy, field, source, classes, boundary, conductance, angles, strengths):
    depth, _, _, rows, width = field.shape
    f32 = jnp.float32
    block = pltpu.VMEM(field.shape, f32)
    flat = (depth, rows, width)
    line = (2, 3, rows, width)
    pair = (2, rows, width)
    dma = pltpu.SemaphoreType.DMA
    hbm = pl.BlockSpec(memory_space=pl.ANY)
    smem = pl.BlockSpec(memory_space=pltpu.SMEM)
    return pl.pallas_call(
        functools.partial(relax, ngz, nxy),
        out_shape=pltpu.VMEM(field.shape, f32),
        in_specs=[hbm] * 4 + [smem] * 3,
        out_specs=pl.BlockSpec(memory_space=pltpu.VMEM),
        scratch_shapes=[
            block,
            block,
            pltpu.VMEM(flat, jnp.int32),
            pltpu.VMEM(flat, jnp.int32),
            pltpu.VMEM(flat, f32),
            pltpu.VMEM(flat, f32),
            block,
            block,
            block,
            block,
            pltpu.VMEM((3, 3, rows, 128), f32),
            pltpu.VMEM((2,) + line, f32),
            pltpu.VMEM((14,) + line, f32),
            pltpu.VMEM((2,) + line, f32),
            pltpu.VMEM((SWEEPS, 2, depth * 6, width), f32),
            pltpu.VMEM((SWEEPS, 2, depth * 6, width), f32),
            pltpu.VMEM((2, 3) + pair, f32),
            pltpu.VMEM((2, 9) + pair, f32),
            pltpu.VMEM((2, 9) + pair, f32),
            pltpu.VMEM((2, 3) + pair, f32),
            pltpu.VMEM((2, 3) + pair, f32),
            pltpu.VMEM((2, 3) + pair, f32),
            pltpu.VMEM((2, 3) + pair, f32),
            pltpu.VMEM((SWEEPS, 2, 3) + pair, f32),
            pltpu.VMEM((SWEEPS, 2, 3) + pair, f32),
            pltpu.VMEM((SWEEPS, 2, 3) + pair, f32),
            pltpu.VMEM((SWEEPS, 2, 3) + pair, f32),
            dma((4,)),
            dma((SWEEPS, 2, PIECES)),
            dma((SWEEPS, 2, PIECES)),
            dma((2, 9)),
            dma((2, 9)),
            dma((2, 2, 3)),
            dma((2, 3)),
            dma((2, 3)),
            dma((2, 3)),
            dma((SWEEPS, 2, 3)),
            dma((SWEEPS, 2, 3)),
            dma((SWEEPS, 2, 2, 3)),
            dma((SWEEPS, 2, 3)),
        ],
        compiler_params=pltpu.CompilerParams(collective_id=0, has_side_effects=True, vmem_limit_bytes=VMEM_LIMIT),
    )(field, source, classes, boundary, conductance, angles, strengths)


def solution(mesh):
    in_specs = (
        P("gz", None, None, "xy", None),
        P("gz", None, None, "xy", None),
        P("gz", "xy", None),
        P("gz", "xy", None),
        P(),
        P(),
        P(),
    )
    out_specs = P("gz", None, None, "xy", None)
    body = functools.partial(local, mesh.shape["gz"], mesh.shape["xy"])
    return jax.shard_map(body, mesh=mesh, in_specs=in_specs, out_specs=out_specs, check_vma=False)
```

```python
import functools

import jax
import jax.numpy as jnp
from jax import lax
from jax.experimental import pallas as pl
from jax.experimental.pallas import tpu as pltpu
from jax.sharding import PartitionSpec as P

SWEEPS = 2
PIECES = 2
VMEM_LIMIT = 62 * 2**20

coupling = 0.1
penalty = 4.0


def mul(a, b):
    return (a[0] * b[0] - a[1] * b[1], a[0] * b[1] + a[1] * b[0])


def add(a, b):
    return (a[0] + b[0], a[1] + b[1])


def inv(a):
    weight = 1.0 / (a[0] * a[0] + a[1] * a[1])
    return (a[0] * weight, -a[1] * weight)


def one_minus(a):
    return (1.0 - a[0], -a[1])


def get(ref, *at):
    return (ref[at + (0,)], ref[at + (1,)])


def put(ref, value, *at):
    ref[at + (0,)] = value[0]
    ref[at + (1,)] = value[1]


def loop(low, high, body, carry, by):
    by = by if (high - low) % by == 0 else 1

    def several(k, carry):
        for i in range(by):
            carry = body(low + k * by + i, carry)
        return carry

    return lax.fori_loop(0, (high - low) // by, several, carry)


def rotation(angles, shape):
    cos = [jnp.cos(jnp.full(shape, angles[i], jnp.float32)) for i in range(3)]
    sin = [jnp.sin(jnp.full(shape, angles[i], jnp.float32)) for i in range(3)]
    (ca, cb, cc), (sa, sb, sc) = cos, sin
    left = [[ca * cb, -sa, ca * sb], [sa * cb, ca, sa * sb], [-sb, jnp.zeros_like(cb), cb]]
    return [[row[0] * cc + row[1] * sc, row[1] * cc - row[0] * sc, row[2]] for row in left]


def relax(
    ngz,
    nxy,
    field,
    source,
    classes,
    boundary,
    conductance,
    angles,
    strengths,
    OUT,
    U,
    S,
    C,
    B,
    SG,
    DR,
    PH,
    PHI,
    PSI,
    T,
    QM,
    EPHI,
    EPSI,
    EH,
    ET,
    ends,
    coef,
    near,
    halo_out,
    halo_in,
    value_in,
    info_in,
    info_out,
    lam_in,
    lam_out,
    extra_in,
    extra_out,
    own_in,
    own_out,
    ch_in,
    ch_out,
    in_sems,
    halo_send,
    halo_recv,
    info_send,
    info_recv,
    lam_send,
    lam_recv,
    extra_send,
    extra_recv,
    own_send,
    own_recv,
    ch_send,
    ch_recv,
):
    ix, iz = lax.axis_index("xy"), lax.axis_index("gz")
    depth, _, _, rows, width = U.shape
    kinds = conductance.shape[0]
    plane = (rows, width)
    has = {
        ("xy", 0): ix > 0,
        ("xy", 1): ix < nxy - 1,
    }
    where_is = {
        ("xy", 0): ix - 1,
        ("xy", 1): ix + 1,
    }
    for steps in (1, 2):
        has["gz", -steps] = iz >= steps
        has["gz", steps] = iz < ngz - steps
        where_is["gz", -steps] = iz - steps
        where_is["gz", steps] = iz + steps
    zs = depth // PIECES
    spans = [pl.ds(piece * zs, zs) for piece in range(PIECES)]
    moves = [(field.at[span], U.at[span]) for span in spans]
    moves += [(classes, C), (boundary, B), (source, S)]
    loads = [
        pltpu.make_async_copy(src, dst, in_sems.at[i]) for i, (src, dst) in enumerate(moves)
    ]
    for load in loads:
        load.start()

    barrier = pltpu.get_barrier_semaphore()
    for key, there in has.items():

        @pl.when(there)
        def _():
            pl.semaphore_signal(
                barrier,
                inc=1,
                device_id={key[0]: where_is[key]},
                device_id_type=pl.DeviceIdType.MESH,
            )


    def remote(src, dst, send, recv, key):
        return pltpu.make_async_remote_copy(
            src_ref=src,
            dst_ref=dst,
            send_sem=send,
            recv_sem=recv,
            device_id={key[0]: where_is[key]},
            device_id_type=pl.DeviceIdType.MESH,
        )

    def halo_copy(sweep, side, piece):
        span = pl.ds(piece * zs, zs)
        return remote(
            halo_out.at[sweep, side, :, :, span],
            halo_in.at[sweep, side, :, :, span],
            halo_send.at[sweep, side, piece],
            halo_recv.at[sweep, side, piece],
            ("xy", 1 - side),
        )

    def send_halo(sweep, piece):
        for side in range(2):

            @pl.when(has["xy", 1 - side])
            def _():
                halo_copy(sweep, side, piece).start()

    def pack(first, last, z, values):
        for i in range(6):
            at = (i // 3, i % 3, pl.ds(z, 1), slice(None))
            first[at] = values[i][:1, :]
            last[at] = values[i][rows - 1 :, :]

    for side in range(2):

        @pl.when(jnp.logical_not(has["xy", side]))
        def _():
            for sweep in range(SWEEPS):
                halo_in[sweep, side] = jnp.zeros(halo_in.shape[2:], jnp.float32)

        @pl.when((iz if side == 0 else ngz - 1 - iz) < 2)
        def _():
            for part in range(3, 9):
                info_in[side, part] = jnp.zeros(info_in.shape[2:], jnp.float32)
            extra_in[side] = jnp.zeros(extra_in.shape[1:], jnp.float32)
            lam_in[side] = jnp.zeros(lam_in.shape[1:], jnp.float32)
            for sweep in range(SWEEPS):
                for j in range(3):
                    ch_in[sweep, side, j] = jnp.zeros(ch_in.shape[3:], jnp.float32)

    count = sum(there.astype(jnp.int32) for there in has.values())

    def pack_first(z, carry):
        values = [U[z, i // 3, i % 3] for i in range(6)]
        pack(halo_out.at[0, 1], halo_out.at[0, 0], z, values)
        return carry

    for piece in range(PIECES):
        loads[piece].wait()
        loop(piece * zs, (piece + 1) * zs, pack_first, 0, 4)
        if piece == 0:
            pl.semaphore_wait(barrier, count)
        send_halo(0, piece)

    loads[PIECES].wait()
    loads[PIECES + 1].wait()

    def diagonal(z, carry):
        ids = C[z]
        sigma = jnp.zeros(plane, jnp.float32)
        for kind in range(kinds):
            sigma = jnp.where(ids == kind, conductance[kind], sigma)
        SG[z] = sigma
        DR[z] = 2.0 + 4.0 * coupling + penalty * B[z].astype(jnp.float32)
        return carry

    loop(0, depth, diagonal, 0, 4)

    def diag(z):
        real = jnp.broadcast_to(DR[z][None], (3,) + plane)
        sigma = SG[z]
        return real, jnp.stack([sigma * strengths[j] for j in range(3)])

    none = (jnp.zeros((3,) + plane, jnp.float32),) * 2

    def pivots(k, carry):
        p, q = carry
        z, back = k, depth - 1 - k
        d, f = diag(z), diag(back)
        p = inv((d[0] - p[0], d[1] - p[1]))
        q = inv((f[0] - q[0], f[1] - q[1]))
        put(PH, p, z)
        put(PHI, q, back)
        return p, q

    loop(0, depth, pivots, (none, none), 2)
    ones = (jnp.ones((3,) + plane, jnp.float32), none[0])

    def columns(k, carry):
        down, up = carry
        z, back = k, depth - 1 - k
        down = mul(get(PHI, z), down)
        up = mul(get(PH, back), up)
        put(PHI, down, z)
        put(PSI, up, back)
        return down, up

    loop(0, depth, columns, (ones, ones), 2)
    LEFT, RIGHT = 0, 1
    tip = (lambda: get(PHI, 0), lambda: get(PSI, depth - 1))
    across = lambda: get(PSI, 0)

    place = (iz, ngz - 1 - iz)
    even = [lax.rem(k, 2) == 0 for k in place]
    odd = [lax.rem(k, 2) == 1 for k in place]
    onward = [ngz - 1 - k for k in place]

    def to(side, steps):
        return {"gz": iz + steps if side == LEFT else iz - steps}

    def chain_copy(src, dst, send, recv, side, steps):
        return pltpu.make_async_remote_copy(
            src_ref=src,
            dst_ref=dst,
            send_sem=send,
            recv_sem=recv,
            device_id=to(side, steps),
            device_id_type=pl.DeviceIdType.MESH,
        )

    def info_copy(side, j):
        return chain_copy(
            info_out.at[side, j],
            info_in.at[side, j],
            info_send.at[side, j],
            info_recv.at[side, j],
            side,
            1,
        )

    def lam_copy(side, steps, j):
        return chain_copy(
            lam_out.at[side, j],
            lam_in.at[side, j],
            lam_send.at[side, steps - 1, j],
            lam_recv.at[side, j],
            side,
            steps,
        )

    def own_copy(sweep, side, j):
        return chain_copy(
            own_out.at[sweep, side, j],
            own_in.at[sweep, side, j],
            own_send.at[sweep, side, j],
            own_recv.at[sweep, side, j],
            side,
            1,
        )

    def x_copy(sweep, side, steps, j):
        return chain_copy(
            ch_out.at[sweep, side, j],
            ch_in.at[sweep, side, j],
            ch_send.at[sweep, side, steps - 1, j],
            ch_recv.at[sweep, side, j],
            side,
            steps,
        )

    both = jnp.logical_and

    def send_info(side):
        parts = (tip[1 - side](), tip[side](), across())
        for part in range(3):
            for j in range(3):
                for p in range(2):
                    info_out[side, part * 3 + j, p] = parts[part][p][j]
            sends = both(even[side], onward[side] >= 1)

            @pl.when(sends if part == 0 else both(sends, place[side] > 0))
            def _():
                for j in range(3):
                    info_copy(side, part * 3 + j).start()

    def pass_lam(side):
        @pl.when(odd[side])
        def _():
            for j in range(3):
                info_copy(side, j).wait_recv()

        @pl.when(both(odd[side], place[side] >= 2))
        def _():
            for j in range(3, 9):
                info_copy(side, j).wait_recv()

        @pl.when(place[side] >= 2)
        def _():
            for j in range(3):
                lam_copy(side, 1, j).wait_recv()

        for j in range(3):
            tips = [(info_in[side, 3 * k + j, 0], info_in[side, 3 * k + j, 1]) for k in range(3)]
            given = (lam_in[side, j, 0], lam_in[side, j, 1])

            @pl.when(odd[side])
            def _():
                skip = mul(tips[2], inv(one_minus(mul(tips[1], given))))
                along = mul(skip, given)
                lam = add(tips[0], mul(tips[2], along))
                for p in range(2):
                    coef[12 + side, p, j] = along[p]
                    coef[8 + side, p, j] = skip[p]
                    coef[10 + side, p, j] = lam[p]

            @pl.when(even[side])
            def _():
                for p in range(2):
                    coef[10 + side, p, j] = given[p]

            of = lambda pair: (pair[0][j], pair[1][j])
            lam = (coef[10 + side, 0, j], coef[10 + side, 1, j])
            kappa = mul(of(across()), inv(one_minus(mul(of(tip[side]()), lam))))
            over = mul(kappa, lam)
            value = add(of(tip[1 - side]()), mul(of(across()), over))
            for p in range(2):
                coef[side, p, j] = kappa[p]
                coef[2 + side, p, j] = over[p]
                lam_out[side, j, p] = value[p]

            for steps in (2, 1):

                @pl.when(both(odd[side], onward[side] >= steps))
                def _():
                    lam_copy(side, steps, j).start()

    def extra_copy(side, j):
        return chain_copy(
            extra_out.at[side, j],
            extra_in.at[side, j],
            extra_send.at[side, j],
            extra_recv.at[side, j],
            side,
            1,
        )

    def own_base(side, j):
        return add(
            (ends[1 - side, 0, j], ends[1 - side, 1, j]),
            mul(
                (coef[2 + side, 0, j], coef[2 + side, 1, j]),
                (ends[side, 0, j], ends[side, 1, j]),
            ),
        )

    def own_sum(sweep, side):
        for j in range(3):
            if sweep == 0:
                for p in range(2):
                    own_out[sweep, side, j, p] = ends[1 - side, p, j]
                    extra_out[side, j, p] = ends[side, p, j]
            else:
                base = own_base(side, j)
                for p in range(2):
                    own_out[sweep, side, j, p] = base[p]
            sends = both(even[side], onward[side] >= 1)

            @pl.when(sends)
            def _():
                own_copy(sweep, side, j).start()

            if sweep == 0:

                @pl.when(both(sends, place[side] > 0))
                def _():
                    extra_copy(side, j).start()

    def pass_chain(sweep, side):
        for j in range(3):
            base = own_base(side, j)

            @pl.when(odd[side])
            def _():
                own_copy(sweep, side, j).wait_recv()

            if sweep == 0:

                @pl.when(both(odd[side], place[side] >= 2))
                def _():
                    extra_copy(side, j).wait_recv()

            @pl.when(place[side] >= 2)
            def _():
                x_copy(sweep, side, 1, j).wait_recv()

            given = (ch_in[sweep, side, j, 0], ch_in[sweep, side, j, 1])

            @pl.when(odd[side])
            def _():
                own = (own_in[sweep, side, j, 0], own_in[sweep, side, j, 1])
                if sweep == 0:
                    extra = (extra_in[side, j, 0], extra_in[side, j, 1])
                    own = add(own, mul((coef[12 + side, 0, j], coef[12 + side, 1, j]), extra))
                x = add(own, mul((coef[8 + side, 0, j], coef[8 + side, 1, j]), given))
                for p in range(2):
                    value_in[side, j, p] = x[p]

            @pl.when(even[side])
            def _():
                for p in range(2):
                    value_in[side, j, p] = given[p]

            x = (value_in[side, j, 0], value_in[side, j, 1])
            result = add(base, mul((coef[side, 0, j], coef[side, 1, j]), x))
            for p in range(2):
                ch_out[sweep, side, j, p] = result[p]

            @pl.when(both(odd[side], onward[side] >= 2))
            def _():
                x_copy(sweep, side, 2, j).start()

        @pl.when(both(odd[side], onward[side] >= 1))
        def _():
            for j in range(3):
                x_copy(sweep, side, 1, j).start()

    left_first = iz * 2 < ngz - 1

    def near_side(run):
        @pl.when(left_first)
        def _():
            run(LEFT)

        @pl.when(jnp.logical_not(left_first))
        def _():
            run(RIGHT)

    def far_side(run):
        @pl.when(left_first)
        def _():
            run(RIGHT)

        @pl.when(jnp.logical_not(left_first))
        def _():
            run(LEFT)

    near_side(send_info)
    far_side(send_info)

    angle_matrix = rotation(angles, (rows, 128))
    for c in range(3):
        for j in range(3):
            QM[c, j] = angle_matrix[c][j]

    def matrix():
        return [
            [jnp.concatenate([QM[c, j]] * (width // 128), axis=1) for j in range(3)]
            for c in range(3)
        ]

    def pack_columns(z, carry):
        for src, dst in ((PHI, EPHI), (PSI, EPSI)):
            pack(dst.at[0], dst.at[1], z, [src[z, i // 3, i % 3] for i in range(6)])
        return carry

    loop(0, depth, pack_columns, 0, 4)

    row = lax.broadcasted_iota(jnp.int32, plane, 0)
    lane = lax.broadcasted_iota(jnp.int32, plane, 1)
    zero = jnp.zeros(plane, jnp.float32)

    def turn(q, driven):
        return [
            jnp.stack(
                [
                    q[0][j] * driven[p][0] + q[1][j] * driven[p][1] + q[2][j] * driven[p][2]
                    for j in range(3)
                ]
            )
            for p in range(2)
        ]

    def inner(z, carry):
        first, last = carry
        q = matrix()
        driven = []
        for p in range(2):
            of = []
            for c in range(3):
                u = U[z, p, c]
                beside = jnp.where(lane == 0, zero, pltpu.roll(u, 1, 1))
                beside += jnp.where(lane == width - 1, zero, pltpu.roll(u, width - 1, 1))
                beside += jnp.where(row == 0, zero, pltpu.roll(u, 1, 0))
                beside += jnp.where(row == rows - 1, zero, pltpu.roll(u, rows - 1, 0))
                of.append(S[z, p, c] + coupling * beside)
            driven.append(of)
        turned = turn(q, driven)
        put(T, turned, z)
        return add(first, mul(get(PHI, z), turned)), add(last, mul(get(PSI, z), turned))

    tiles = [pl.ds(z, rows) for z in range(0, depth, rows)]

    def outer(sweep, side, tile, carry):
        first, last = carry
        q = matrix()
        turned = turn(
            q,
            [[coupling * halo_in[sweep, side, p, c, tile] for c in range(3)] for p in range(2)],
        )
        for p in range(2):
            EH[side, p, :, tile] = turned[p]
        phi = [EPHI[side, p, :, tile] for p in range(2)]
        psi = [EPSI[side, p, :, tile] for p in range(2)]
        return add(first, mul(phi, turned)), add(last, mul(psi, turned))

    loads[PIECES + 2].wait()
    for sweep in range(SWEEPS):
        sums = loop(0, depth, inner, (none, none), 4)
        halves = [(none, none), (none, none)]
        for piece in range(PIECES):
            for side in range(2):

                @pl.when(has["xy", side])
                def _():
                    halo_copy(sweep, side, piece).wait_recv()

                for tile in tiles[piece * len(tiles) // PIECES : (piece + 1) * len(tiles) // PIECES]:
                    halves[side] = outer(sweep, side, tile, halves[side])
        for side in range(2):
            here = row == (0 if side == 0 else rows - 1)
            sums = tuple(
                add(
                    sums[end],
                    tuple(
                        jnp.where(here[None], jnp.sum(part, axis=1, keepdims=True), 0.0)
                        for part in halves[side][end]
                    ),
                )
                for end in range(2)
            )
        put(ends, sums[0], 0)
        put(ends, sums[1], 1)

        near_side(functools.partial(own_sum, sweep))
        far_side(functools.partial(own_sum, sweep))
        if sweep == 0:
            near_side(pass_lam)
        near_side(functools.partial(pass_chain, sweep))

        def forward(z, m):
            given = []
            for p in range(2):
                edges = []
                for j in range(3):
                    above = jnp.broadcast_to(EH[0, p, j, pl.ds(z, 1), :], plane)
                    below = jnp.broadcast_to(EH[1, p, j, pl.ds(z, 1), :], plane)
                    edges.append(
                        jnp.where(row == 0, above, zero) + jnp.where(row == rows - 1, below, zero)
                    )
                given.append(T[z, p] + jnp.stack(edges))
            m = mul(get(PH, z), add(given, m))
            put(T, m, z)
            return m

        def backward(k, w):
            z = depth - 1 - k
            w = add(get(T, z), mul(get(PH, z), w))
            put(T, w, z)
            if sweep < SWEEPS - 1:
                pack(ET.at[0], ET.at[1], z, [w[i // 3][i % 3] for i in range(6)])
            return w

        loop(0, depth, forward, none, 4)
        loop(0, depth, backward, none, 4)
        if sweep == 0:
            far_side(pass_lam)
            for side in range(2):
                lam = get(coef, 10 + side)
                away = tuple(
                    jnp.stack([lam_out[1 - side, j, p] for j in range(3)]) for p in range(2)
                )
                det = inv(one_minus(mul(lam, away)))
                put(coef, det, 6 + side)
                put(coef, mul(det, lam), 4 + side)
        far_side(functools.partial(pass_chain, sweep))

        for side in range(2):
            for j in range(3):
                arrived = (value_in[side, j, 0], value_in[side, j, 1])
                other = (ch_out[sweep, 1 - side, j, 0], ch_out[sweep, 1 - side, j, 1])
                value = add(
                    mul((coef[6 + side, 0, j], coef[6 + side, 1, j]), arrived),
                    mul((coef[4 + side, 0, j], coef[4 + side, 1, j]), other),
                )
                near[side, 0, j] = value[0]
                near[side, 1, j] = value[1]

        final = sweep == SWEEPS - 1

        def join_edge(side, tile):
            q = matrix()
            r = 0 if side == 0 else rows - 1
            w = [ET[side, p, :, tile] for p in range(2)]
            for end, column in ((0, EPHI), (1, EPSI)):
                entry = [
                    jnp.broadcast_to(near[end, p, :, r : r + 1, :], (3,) + plane)
                    for p in range(2)
                ]
                w = add(w, mul([column[side, p, :, tile] for p in range(2)], entry))
            for p in range(2):
                for c in range(3):
                    halo_out[sweep + 1, 1 - side, p, c, tile] = (
                        q[c][0] * w[p][0] + q[c][1] * w[p][1] + q[c][2] * w[p][2]
                    )

        if not final:
            for piece in range(PIECES):
                for tile in tiles[piece * len(tiles) // PIECES : (piece + 1) * len(tiles) // PIECES]:
                    for side in range(2):
                        join_edge(side, tile)
                send_halo(sweep + 1, piece)


        def join(z, carry):
            q = matrix()
            before, after = get(near, 0), get(near, 1)
            w = add(add(get(T, z), mul(get(PHI, z), before)), mul(get(PSI, z), after))
            values = []
            for p in range(2):
                for c in range(3):
                    values.append(q[c][0] * w[p][0] + q[c][1] * w[p][1] + q[c][2] * w[p][2])
            target = OUT if final else U
            for i in range(6):
                target[z, i // 3, i % 3] = values[i]
            return carry

        loop(0, depth, join, 0, 4)

    for side in range(2):

        @pl.when(has["xy", 1 - side])
        def _():
            for sweep in range(SWEEPS):
                for piece in range(PIECES):
                    halo_copy(sweep, side, piece).wait_send()

        sends = both(even[side], onward[side] >= 1)

        @pl.when(sends)
        def _():
            for j in range(3):
                info_copy(side, j).wait_send()
                for sweep in range(SWEEPS):
                    own_copy(sweep, side, j).wait_send()

        @pl.when(both(sends, place[side] > 0))
        def _():
            for j in range(3, 9):
                info_copy(side, j).wait_send()
            for j in range(3):
                extra_copy(side, j).wait_send()

        for steps in (2, 1):

            @pl.when(both(odd[side], onward[side] >= steps))
            def _():
                for j in range(3):
                    lam_copy(side, steps, j).wait_send()
                    for sweep in range(SWEEPS):
                        x_copy(sweep, side, steps, j).wait_send()


def local(ngz, nxy, field, source, classes, boundary, conductance, angles, strengths):
    depth, _, _, rows, width = field.shape
    f32 = jnp.float32
    block = pltpu.VMEM(field.shape, f32)
    flat = (depth, rows, width)
    line = (2, 3, rows, width)
    pair = (2, rows, width)
    edge = (2, 2, 3, depth, width)
    dma = pltpu.SemaphoreType.DMA
    hbm = pl.BlockSpec(memory_space=pl.ANY)
    smem = pl.BlockSpec(memory_space=pltpu.SMEM)
    return pl.pallas_call(
        functools.partial(relax, ngz, nxy),
        out_shape=pltpu.VMEM(field.shape, f32),
        in_specs=[hbm] * 4 + [smem] * 3,
        out_specs=pl.BlockSpec(memory_space=pltpu.VMEM),
        scratch_shapes=[
            block,
            block,
            pltpu.VMEM(flat, jnp.int32),
            pltpu.VMEM(flat, jnp.int32),
            pltpu.VMEM(flat, f32),
            pltpu.VMEM(flat, f32),
            block,
            block,
            block,
            block,
            pltpu.VMEM((3, 3, rows, 128), f32),
            pltpu.VMEM(edge, f32),
            pltpu.VMEM(edge, f32),
            pltpu.VMEM(edge, f32),
            pltpu.VMEM(edge, f32),
            pltpu.VMEM((2,) + line, f32),
            pltpu.VMEM((14,) + line, f32),
            pltpu.VMEM((2,) + line, f32),
            pltpu.VMEM((SWEEPS,) + edge, f32),
            pltpu.VMEM((SWEEPS,) + edge, f32),
            pltpu.VMEM((2, 3) + pair, f32),
            pltpu.VMEM((2, 9) + pair, f32),
            pltpu.VMEM((2, 9) + pair, f32),
            pltpu.VMEM((2, 3) + pair, f32),
            pltpu.VMEM((2, 3) + pair, f32),
            pltpu.VMEM((2, 3) + pair, f32),
            pltpu.VMEM((2, 3) + pair, f32),
            pltpu.VMEM((SWEEPS, 2, 3) + pair, f32),
            pltpu.VMEM((SWEEPS, 2, 3) + pair, f32),
            pltpu.VMEM((SWEEPS, 2, 3) + pair, f32),
            pltpu.VMEM((SWEEPS, 2, 3) + pair, f32),
            dma((PIECES + 3,)),
            dma((SWEEPS, 2, PIECES)),
            dma((SWEEPS, 2, PIECES)),
            dma((2, 9)),
            dma((2, 9)),
            dma((2, 2, 3)),
            dma((2, 3)),
            dma((2, 3)),
            dma((2, 3)),
            dma((SWEEPS, 2, 3)),
            dma((SWEEPS, 2, 3)),
            dma((SWEEPS, 2, 2, 3)),
            dma((SWEEPS, 2, 3)),
        ],
        compiler_params=pltpu.CompilerParams(collective_id=0, has_side_effects=True, vmem_limit_bytes=VMEM_LIMIT),
    )(field, source, classes, boundary, conductance, angles, strengths)


def solution(mesh):
    in_specs = (
        P("gz", None, None, "xy", None),
        P("gz", None, None, "xy", None),
        P("gz", "xy", None),
        P("gz", "xy", None),
        P(),
        P(),
        P(),
    )
    out_specs = P("gz", None, None, "xy", None)
    body = functools.partial(local, mesh.shape["gz"], mesh.shape["xy"])
    return jax.shard_map(body, mesh=mesh, in_specs=in_specs, out_specs=out_specs, check_vma=False)
```

```python
import functools

import jax
import jax.numpy as jnp
from jax import lax
from jax.experimental import pallas as pl
from jax.experimental.pallas import tpu as pltpu
from jax.sharding import PartitionSpec as P

SWEEPS = 2
PIECES = 2
VMEM_LIMIT = 62 * 2**20

coupling = 0.1
penalty = 4.0


def mul(a, b):
    return (a[0] * b[0] - a[1] * b[1], a[0] * b[1] + a[1] * b[0])


def add(a, b):
    return (a[0] + b[0], a[1] + b[1])


def inv(a):
    weight = 1.0 / (a[0] * a[0] + a[1] * a[1])
    return (a[0] * weight, -a[1] * weight)


def one_minus(a):
    return (1.0 - a[0], -a[1])


def get(ref, *at):
    return (ref[at + (0,)], ref[at + (1,)])


def put(ref, value, *at):
    ref[at + (0,)] = value[0]
    ref[at + (1,)] = value[1]


def loop(low, high, body, carry, by):
    by = by if (high - low) % by == 0 else 1

    def several(k, carry):
        for i in range(by):
            carry = body(low + k * by + i, carry)
        return carry

    return lax.fori_loop(0, (high - low) // by, several, carry)


def rotation(angles, shape):
    cos = [jnp.cos(jnp.full(shape, angles[i], jnp.float32)) for i in range(3)]
    sin = [jnp.sin(jnp.full(shape, angles[i], jnp.float32)) for i in range(3)]
    (ca, cb, cc), (sa, sb, sc) = cos, sin
    left = [[ca * cb, -sa, ca * sb], [sa * cb, ca, sa * sb], [-sb, jnp.zeros_like(cb), cb]]
    return [[row[0] * cc + row[1] * sc, row[1] * cc - row[0] * sc, row[2]] for row in left]


def relax(
    ngz,
    nxy,
    field,
    source,
    classes,
    boundary,
    conductance,
    angles,
    strengths,
    OUT,
    U,
    S,
    C,
    B,
    SG,
    DR,
    PH,
    PHI,
    PSI,
    T,
    QM,
    EPHI,
    EPSI,
    EH,
    ET,
    ends,
    coef,
    near,
    halo_out,
    halo_in,
    value_in,
    info_in,
    info_out,
    lam_in,
    lam_out,
    extra_in,
    extra_out,
    own_in,
    own_out,
    ch_in,
    ch_out,
    in_sems,
    halo_send,
    halo_recv,
    info_send,
    info_recv,
    lam_send,
    lam_recv,
    extra_send,
    extra_recv,
    own_send,
    own_recv,
    ch_send,
    ch_recv,
):
    ix, iz = lax.axis_index("xy"), lax.axis_index("gz")
    depth, _, _, rows, width = U.shape
    kinds = conductance.shape[0]
    plane = (rows, width)
    has = {
        ("xy", 0): ix > 0,
        ("xy", 1): ix < nxy - 1,
    }
    where_is = {
        ("xy", 0): ix - 1,
        ("xy", 1): ix + 1,
    }
    for steps in (1, 2):
        has["gz", -steps] = iz >= steps
        has["gz", steps] = iz < ngz - steps
        where_is["gz", -steps] = iz - steps
        where_is["gz", steps] = iz + steps
    zs = depth // PIECES
    spans = [pl.ds(piece * zs, zs) for piece in range(PIECES)]
    moves = [(field.at[span], U.at[span]) for span in spans]
    moves += [(classes, C), (boundary, B), (source, S)]
    loads = [
        pltpu.make_async_copy(src, dst, in_sems.at[i]) for i, (src, dst) in enumerate(moves)
    ]
    for load in loads[:-1]:
        load.start()

    barrier = pltpu.get_barrier_semaphore()
    for key, there in has.items():

        @pl.when(there)
        def _():
            pl.semaphore_signal(
                barrier,
                inc=1,
                device_id={key[0]: where_is[key]},
                device_id_type=pl.DeviceIdType.MESH,
            )


    def remote(src, dst, send, recv, key):
        return pltpu.make_async_remote_copy(
            src_ref=src,
            dst_ref=dst,
            send_sem=send,
            recv_sem=recv,
            device_id={key[0]: where_is[key]},
            device_id_type=pl.DeviceIdType.MESH,
        )

    def halo_copy(sweep, side, piece):
        span = pl.ds(piece * zs, zs)
        return remote(
            halo_out.at[sweep, side, :, :, span],
            halo_in.at[sweep, side, :, :, span],
            halo_send.at[sweep, side, piece],
            halo_recv.at[sweep, side, piece],
            ("xy", 1 - side),
        )

    def send_halo(sweep, piece):
        for side in range(2):

            @pl.when(has["xy", 1 - side])
            def _():
                halo_copy(sweep, side, piece).start()

    def pack(first, last, z, values):
        for i in range(6):
            at = (i // 3, i % 3, pl.ds(z, 1), slice(None))
            first[at] = values[i][:1, :]
            last[at] = values[i][rows - 1 :, :]

    for side in range(2):

        @pl.when(jnp.logical_not(has["xy", side]))
        def _():
            for sweep in range(SWEEPS):
                halo_in[sweep, side] = jnp.zeros(halo_in.shape[2:], jnp.float32)

        @pl.when((iz if side == 0 else ngz - 1 - iz) < 2)
        def _():
            for part in range(3, 9):
                info_in[side, part] = jnp.zeros(info_in.shape[2:], jnp.float32)
            extra_in[side] = jnp.zeros(extra_in.shape[1:], jnp.float32)
            lam_in[side] = jnp.zeros(lam_in.shape[1:], jnp.float32)
            for sweep in range(SWEEPS):
                for j in range(3):
                    ch_in[sweep, side, j] = jnp.zeros(ch_in.shape[3:], jnp.float32)

    count = sum(there.astype(jnp.int32) for there in has.values())

    def pack_first(z, carry):
        values = [U[z, i // 3, i % 3] for i in range(6)]
        pack(halo_out.at[0, 1], halo_out.at[0, 0], z, values)
        return carry

    for piece in range(PIECES):
        loads[piece].wait()
        if piece == PIECES - 1:
            loads[-1].start()
        loop(piece * zs, (piece + 1) * zs, pack_first, 0, 4)
        if piece == 0:
            pl.semaphore_wait(barrier, count)
        send_halo(0, piece)

    loads[PIECES].wait()
    loads[PIECES + 1].wait()

    def diagonal(z, carry):
        ids = C[z]
        sigma = jnp.zeros(plane, jnp.float32)
        for kind in range(kinds):
            sigma = jnp.where(ids == kind, conductance[kind], sigma)
        SG[z] = sigma
        DR[z] = 2.0 + 4.0 * coupling + penalty * B[z].astype(jnp.float32)
        return carry

    loop(0, depth, diagonal, 0, 4)

    def diag(z):
        real = jnp.broadcast_to(DR[z][None], (3,) + plane)
        sigma = SG[z]
        return real, jnp.stack([sigma * strengths[j] for j in range(3)])

    none = (jnp.zeros((3,) + plane, jnp.float32),) * 2

    def pivots(k, carry):
        p, q = carry
        z, back = k, depth - 1 - k
        d, f = diag(z), diag(back)
        p = inv((d[0] - p[0], d[1] - p[1]))
        q = inv((f[0] - q[0], f[1] - q[1]))
        put(PH, p, z)
        put(PHI, q, back)
        return p, q

    loop(0, depth, pivots, (none, none), 2)
    ones = (jnp.ones((3,) + plane, jnp.float32), none[0])

    def columns(k, carry):
        down, up = carry
        z, back = k, depth - 1 - k
        down = mul(get(PHI, z), down)
        up = mul(get(PH, back), up)
        put(PHI, down, z)
        put(PSI, up, back)
        return down, up

    loop(0, depth, columns, (ones, ones), 2)
    LEFT, RIGHT = 0, 1
    tip = (lambda: get(PHI, 0), lambda: get(PSI, depth - 1))
    across = lambda: get(PSI, 0)

    place = (iz, ngz - 1 - iz)
    even = [lax.rem(k, 2) == 0 for k in place]
    odd = [lax.rem(k, 2) == 1 for k in place]
    onward = [ngz - 1 - k for k in place]

    def to(side, steps):
        return {"gz": iz + steps if side == LEFT else iz - steps}

    def chain_copy(src, dst, send, recv, side, steps):
        return pltpu.make_async_remote_copy(
            src_ref=src,
            dst_ref=dst,
            send_sem=send,
            recv_sem=recv,
            device_id=to(side, steps),
            device_id_type=pl.DeviceIdType.MESH,
        )

    def info_copy(side, j):
        return chain_copy(
            info_out.at[side, j],
            info_in.at[side, j],
            info_send.at[side, j],
            info_recv.at[side, j],
            side,
            1,
        )

    def lam_copy(side, steps, j):
        return chain_copy(
            lam_out.at[side, j],
            lam_in.at[side, j],
            lam_send.at[side, steps - 1, j],
            lam_recv.at[side, j],
            side,
            steps,
        )

    def own_copy(sweep, side, j):
        return chain_copy(
            own_out.at[sweep, side, j],
            own_in.at[sweep, side, j],
            own_send.at[sweep, side, j],
            own_recv.at[sweep, side, j],
            side,
            1,
        )

    def x_copy(sweep, side, steps, j):
        return chain_copy(
            ch_out.at[sweep, side, j],
            ch_in.at[sweep, side, j],
            ch_send.at[sweep, side, steps - 1, j],
            ch_recv.at[sweep, side, j],
            side,
            steps,
        )

    both = jnp.logical_and

    def send_info(side):
        parts = (tip[1 - side](), tip[side](), across())
        for part in range(3):
            for j in range(3):
                for p in range(2):
                    info_out[side, part * 3 + j, p] = parts[part][p][j]
            sends = both(even[side], onward[side] >= 1)

            @pl.when(sends if part == 0 else both(sends, place[side] > 0))
            def _():
                for j in range(3):
                    info_copy(side, part * 3 + j).start()

    def pass_lam(side):
        @pl.when(odd[side])
        def _():
            for j in range(3):
                info_copy(side, j).wait_recv()

        @pl.when(both(odd[side], place[side] >= 2))
        def _():
            for j in range(3, 9):
                info_copy(side, j).wait_recv()

        @pl.when(place[side] >= 2)
        def _():
            for j in range(3):
                lam_copy(side, 1, j).wait_recv()

        for j in range(3):
            tips = [(info_in[side, 3 * k + j, 0], info_in[side, 3 * k + j, 1]) for k in range(3)]
            given = (lam_in[side, j, 0], lam_in[side, j, 1])

            @pl.when(odd[side])
            def _():
                skip = mul(tips[2], inv(one_minus(mul(tips[1], given))))
                along = mul(skip, given)
                lam = add(tips[0], mul(tips[2], along))
                for p in range(2):
                    coef[12 + side, p, j] = along[p]
                    coef[8 + side, p, j] = skip[p]
                    coef[10 + side, p, j] = lam[p]

            @pl.when(even[side])
            def _():
                for p in range(2):
                    coef[10 + side, p, j] = given[p]

            of = lambda pair: (pair[0][j], pair[1][j])
            lam = (coef[10 + side, 0, j], coef[10 + side, 1, j])
            kappa = mul(of(across()), inv(one_minus(mul(of(tip[side]()), lam))))
            over = mul(kappa, lam)
            value = add(of(tip[1 - side]()), mul(of(across()), over))
            for p in range(2):
                coef[side, p, j] = kappa[p]
                coef[2 + side, p, j] = over[p]
                lam_out[side, j, p] = value[p]

            @pl.when(both(odd[side], onward[side] >= 2))
            def _():
                lam_copy(side, 2, j).start()

        @pl.when(both(odd[side], onward[side] >= 1))
        def _():
            for j in range(3):
                lam_copy(side, 1, j).start()

    def extra_copy(side, j):
        return chain_copy(
            extra_out.at[side, j],
            extra_in.at[side, j],
            extra_send.at[side, j],
            extra_recv.at[side, j],
            side,
            1,
        )

    def own_base(side, j):
        return add(
            (ends[1 - side, 0, j], ends[1 - side, 1, j]),
            mul(
                (coef[2 + side, 0, j], coef[2 + side, 1, j]),
                (ends[side, 0, j], ends[side, 1, j]),
            ),
        )

    def own_sum(sweep, side):
        for j in range(3):
            if sweep == 0:
                for p in range(2):
                    own_out[sweep, side, j, p] = ends[1 - side, p, j]
                    extra_out[side, j, p] = ends[side, p, j]
            else:
                base = own_base(side, j)
                for p in range(2):
                    own_out[sweep, side, j, p] = base[p]
            sends = both(even[side], onward[side] >= 1)

            @pl.when(sends)
            def _():
                own_copy(sweep, side, j).start()

            if sweep == 0:

                @pl.when(both(sends, place[side] > 0))
                def _():
                    extra_copy(side, j).start()

    def pass_chain(sweep, side):
        for j in range(3):
            base = own_base(side, j)

            @pl.when(odd[side])
            def _():
                own_copy(sweep, side, j).wait_recv()

            if sweep == 0:

                @pl.when(both(odd[side], place[side] >= 2))
                def _():
                    extra_copy(side, j).wait_recv()

            @pl.when(place[side] >= 2)
            def _():
                x_copy(sweep, side, 1, j).wait_recv()

            given = (ch_in[sweep, side, j, 0], ch_in[sweep, side, j, 1])

            @pl.when(odd[side])
            def _():
                own = (own_in[sweep, side, j, 0], own_in[sweep, side, j, 1])
                if sweep == 0:
                    extra = (extra_in[side, j, 0], extra_in[side, j, 1])
                    own = add(own, mul((coef[12 + side, 0, j], coef[12 + side, 1, j]), extra))
                x = add(own, mul((coef[8 + side, 0, j], coef[8 + side, 1, j]), given))
                for p in range(2):
                    value_in[side, j, p] = x[p]

            @pl.when(even[side])
            def _():
                for p in range(2):
                    value_in[side, j, p] = given[p]

            x = (value_in[side, j, 0], value_in[side, j, 1])
            result = add(base, mul((coef[side, 0, j], coef[side, 1, j]), x))
            for p in range(2):
                ch_out[sweep, side, j, p] = result[p]

            @pl.when(both(odd[side], onward[side] >= 2))
            def _():
                x_copy(sweep, side, 2, j).start()

        @pl.when(both(odd[side], onward[side] >= 1))
        def _():
            for j in range(3):
                x_copy(sweep, side, 1, j).start()

    left_first = iz * 2 < ngz - 1

    def near_side(run):
        @pl.when(left_first)
        def _():
            run(LEFT)

        @pl.when(jnp.logical_not(left_first))
        def _():
            run(RIGHT)

    def far_side(run):
        @pl.when(left_first)
        def _():
            run(RIGHT)

        @pl.when(jnp.logical_not(left_first))
        def _():
            run(LEFT)

    near_side(send_info)
    far_side(send_info)

    angle_matrix = rotation(angles, (rows, 128))
    for c in range(3):
        for j in range(3):
            QM[c, j] = angle_matrix[c][j]

    def matrix():
        return [
            [jnp.concatenate([QM[c, j]] * (width // 128), axis=1) for j in range(3)]
            for c in range(3)
        ]

    def pack_columns(z, carry):
        for src, dst in ((PHI, EPHI), (PSI, EPSI)):
            pack(dst.at[0], dst.at[1], z, [src[z, i // 3, i % 3] for i in range(6)])
        return carry

    loop(0, depth, pack_columns, 0, 4)

    row = lax.broadcasted_iota(jnp.int32, plane, 0)
    lane = lax.broadcasted_iota(jnp.int32, plane, 1)
    zero = jnp.zeros(plane, jnp.float32)

    def turn(q, driven):
        return [
            jnp.stack(
                [
                    q[0][j] * driven[p][0] + q[1][j] * driven[p][1] + q[2][j] * driven[p][2]
                    for j in range(3)
                ]
            )
            for p in range(2)
        ]

    def inner(z, carry):
        first, last = carry
        q = matrix()
        driven = []
        for p in range(2):
            of = []
            for c in range(3):
                u = U[z, p, c]
                beside = jnp.where(lane == 0, zero, pltpu.roll(u, 1, 1))
                beside += jnp.where(lane == width - 1, zero, pltpu.roll(u, width - 1, 1))
                beside += jnp.where(row == 0, zero, pltpu.roll(u, 1, 0))
                beside += jnp.where(row == rows - 1, zero, pltpu.roll(u, rows - 1, 0))
                of.append(S[z, p, c] + coupling * beside)
            driven.append(of)
        turned = turn(q, driven)
        put(T, turned, z)
        return add(first, mul(get(PHI, z), turned)), add(last, mul(get(PSI, z), turned))

    tiles = [pl.ds(z, rows) for z in range(0, depth, rows)]

    def outer(sweep, side, tile, carry):
        first, last = carry
        q = matrix()
        turned = turn(
            q,
            [[coupling * halo_in[sweep, side, p, c, tile] for c in range(3)] for p in range(2)],
        )
        for p in range(2):
            EH[side, p, :, tile] = turned[p]
        phi = [EPHI[side, p, :, tile] for p in range(2)]
        psi = [EPSI[side, p, :, tile] for p in range(2)]
        return add(first, mul(phi, turned)), add(last, mul(psi, turned))

    loads[PIECES + 2].wait()
    for sweep in range(SWEEPS):
        sums = loop(0, depth, inner, (none, none), 4)
        halves = [(none, none), (none, none)]
        for piece in range(PIECES):
            for side in range(2):

                @pl.when(has["xy", side])
                def _():
                    halo_copy(sweep, side, piece).wait_recv()

                for tile in tiles[piece * len(tiles) // PIECES : (piece + 1) * len(tiles) // PIECES]:
                    halves[side] = outer(sweep, side, tile, halves[side])
        for side in range(2):
            here = row == (0 if side == 0 else rows - 1)
            sums = tuple(
                add(
                    sums[end],
                    tuple(
                        jnp.where(here[None], jnp.sum(part, axis=1, keepdims=True), 0.0)
                        for part in halves[side][end]
                    ),
                )
                for end in range(2)
            )
        put(ends, sums[0], 0)
        put(ends, sums[1], 1)

        near_side(functools.partial(own_sum, sweep))
        far_side(functools.partial(own_sum, sweep))
        if sweep == 0:
            near_side(pass_lam)
        near_side(functools.partial(pass_chain, sweep))

        def forward(z, m):
            given = []
            for p in range(2):
                edges = []
                for j in range(3):
                    above = jnp.broadcast_to(EH[0, p, j, pl.ds(z, 1), :], plane)
                    below = jnp.broadcast_to(EH[1, p, j, pl.ds(z, 1), :], plane)
                    edges.append(
                        jnp.where(row == 0, above, zero) + jnp.where(row == rows - 1, below, zero)
                    )
                given.append(T[z, p] + jnp.stack(edges))
            m = mul(get(PH, z), add(given, m))
            put(T, m, z)
            return m

        def backward(k, w):
            z = depth - 1 - k
            w = add(get(T, z), mul(get(PH, z), w))
            put(T, w, z)
            if sweep < SWEEPS - 1:
                pack(ET.at[0], ET.at[1], z, [w[i // 3][i % 3] for i in range(6)])
            return w

        loop(0, depth, forward, none, 4)
        loop(0, depth, backward, none, 4)
        if sweep == 0:
            far_side(pass_lam)
            for side in range(2):
                lam = get(coef, 10 + side)
                away = tuple(
                    jnp.stack([lam_out[1 - side, j, p] for j in range(3)]) for p in range(2)
                )
                det = inv(one_minus(mul(lam, away)))
                put(coef, det, 6 + side)
                put(coef, mul(det, lam), 4 + side)
        far_side(functools.partial(pass_chain, sweep))

        for side in range(2):
            for j in range(3):
                arrived = (value_in[side, j, 0], value_in[side, j, 1])
                other = (ch_out[sweep, 1 - side, j, 0], ch_out[sweep, 1 - side, j, 1])
                value = add(
                    mul((coef[6 + side, 0, j], coef[6 + side, 1, j]), arrived),
                    mul((coef[4 + side, 0, j], coef[4 + side, 1, j]), other),
                )
                near[side, 0, j] = value[0]
                near[side, 1, j] = value[1]

        final = sweep == SWEEPS - 1

        def join_edge(side, tile):
            q = matrix()
            r = 0 if side == 0 else rows - 1
            w = [ET[side, p, :, tile] for p in range(2)]
            for end, column in ((0, EPHI), (1, EPSI)):
                entry = [
                    jnp.broadcast_to(near[end, p, :, r : r + 1, :], (3,) + plane)
                    for p in range(2)
                ]
                w = add(w, mul([column[side, p, :, tile] for p in range(2)], entry))
            for p in range(2):
                for c in range(3):
                    halo_out[sweep + 1, 1 - side, p, c, tile] = (
                        q[c][0] * w[p][0] + q[c][1] * w[p][1] + q[c][2] * w[p][2]
                    )

        if not final:
            for piece in range(PIECES):
                for tile in tiles[piece * len(tiles) // PIECES : (piece + 1) * len(tiles) // PIECES]:
                    for side in range(2):
                        join_edge(side, tile)
                send_halo(sweep + 1, piece)


        def join(z, carry):
            q = matrix()
            before, after = get(near, 0), get(near, 1)
            w = add(add(get(T, z), mul(get(PHI, z), before)), mul(get(PSI, z), after))
            values = []
            for p in range(2):
                for c in range(3):
                    values.append(q[c][0] * w[p][0] + q[c][1] * w[p][1] + q[c][2] * w[p][2])
            target = OUT if final else U
            for i in range(6):
                target[z, i // 3, i % 3] = values[i]
            return carry

        loop(0, depth, join, 0, 4)

    for side in range(2):

        @pl.when(has["xy", 1 - side])
        def _():
            for sweep in range(SWEEPS):
                for piece in range(PIECES):
                    halo_copy(sweep, side, piece).wait_send()

        sends = both(even[side], onward[side] >= 1)

        @pl.when(sends)
        def _():
            for j in range(3):
                info_copy(side, j).wait_send()
                for sweep in range(SWEEPS):
                    own_copy(sweep, side, j).wait_send()

        @pl.when(both(sends, place[side] > 0))
        def _():
            for j in range(3, 9):
                info_copy(side, j).wait_send()
            for j in range(3):
                extra_copy(side, j).wait_send()

        for steps in (2, 1):

            @pl.when(both(odd[side], onward[side] >= steps))
            def _():
                for j in range(3):
                    lam_copy(side, steps, j).wait_send()
                    for sweep in range(SWEEPS):
                        x_copy(sweep, side, steps, j).wait_send()


def local(ngz, nxy, field, source, classes, boundary, conductance, angles, strengths):
    depth, _, _, rows, width = field.shape
    f32 = jnp.float32
    block = pltpu.VMEM(field.shape, f32)
    flat = (depth, rows, width)
    line = (2, 3, rows, width)
    pair = (2, rows, width)
    edge = (2, 2, 3, depth, width)
    dma = pltpu.SemaphoreType.DMA
    hbm = pl.BlockSpec(memory_space=pl.ANY)
    smem = pl.BlockSpec(memory_space=pltpu.SMEM)
    return pl.pallas_call(
        functools.partial(relax, ngz, nxy),
        out_shape=pltpu.VMEM(field.shape, f32),
        in_specs=[hbm] * 4 + [smem] * 3,
        out_specs=pl.BlockSpec(memory_space=pltpu.VMEM),
        scratch_shapes=[
            block,
            block,
            pltpu.VMEM(flat, jnp.int32),
            pltpu.VMEM(flat, jnp.int32),
            pltpu.VMEM(flat, f32),
            pltpu.VMEM(flat, f32),
            block,
            block,
            block,
            block,
            pltpu.VMEM((3, 3, rows, 128), f32),
            pltpu.VMEM(edge, f32),
            pltpu.VMEM(edge, f32),
            pltpu.VMEM(edge, f32),
            pltpu.VMEM(edge, f32),
            pltpu.VMEM((2,) + line, f32),
            pltpu.VMEM((14,) + line, f32),
            pltpu.VMEM((2,) + line, f32),
            pltpu.VMEM((SWEEPS,) + edge, f32),
            pltpu.VMEM((SWEEPS,) + edge, f32),
            pltpu.VMEM((2, 3) + pair, f32),
            pltpu.VMEM((2, 9) + pair, f32),
            pltpu.VMEM((2, 9) + pair, f32),
            pltpu.VMEM((2, 3) + pair, f32),
            pltpu.VMEM((2, 3) + pair, f32),
            pltpu.VMEM((2, 3) + pair, f32),
            pltpu.VMEM((2, 3) + pair, f32),
            pltpu.VMEM((SWEEPS, 2, 3) + pair, f32),
            pltpu.VMEM((SWEEPS, 2, 3) + pair, f32),
            pltpu.VMEM((SWEEPS, 2, 3) + pair, f32),
            pltpu.VMEM((SWEEPS, 2, 3) + pair, f32),
            dma((PIECES + 3,)),
            dma((SWEEPS, 2, PIECES)),
            dma((SWEEPS, 2, PIECES)),
            dma((2, 9)),
            dma((2, 9)),
            dma((2, 2, 3)),
            dma((2, 3)),
            dma((2, 3)),
            dma((2, 3)),
            dma((SWEEPS, 2, 3)),
            dma((SWEEPS, 2, 3)),
            dma((SWEEPS, 2, 2, 3)),
            dma((SWEEPS, 2, 3)),
        ],
        compiler_params=pltpu.CompilerParams(collective_id=0, has_side_effects=True, vmem_limit_bytes=VMEM_LIMIT),
    )(field, source, classes, boundary, conductance, angles, strengths)


def solution(mesh):
    in_specs = (
        P("gz", None, None, "xy", None),
        P("gz", None, None, "xy", None),
        P("gz", "xy", None),
        P("gz", "xy", None),
        P(),
        P(),
        P(),
    )
    out_specs = P("gz", None, None, "xy", None)
    body = functools.partial(local, mesh.shape["gz"], mesh.shape["xy"])
    return jax.shard_map(body, mesh=mesh, in_specs=in_specs, out_specs=out_specs, check_vma=False)
```

```python
import functools

import jax
import jax.numpy as jnp
from jax import lax
from jax.experimental import pallas as pl
from jax.experimental.pallas import tpu as pltpu
from jax.sharding import PartitionSpec as P

SWEEPS = 2
PIECES = 2
VMEM_LIMIT = 62 * 2**20

coupling = 0.1
penalty = 4.0


def mul(a, b):
    return (a[0] * b[0] - a[1] * b[1], a[0] * b[1] + a[1] * b[0])


def add(a, b):
    return (a[0] + b[0], a[1] + b[1])


def inv(a):
    weight = 1.0 / (a[0] * a[0] + a[1] * a[1])
    return (a[0] * weight, -a[1] * weight)


def one_minus(a):
    return (1.0 - a[0], -a[1])


def get(ref, *at):
    return (ref[at + (0,)], ref[at + (1,)])


def put(ref, value, *at):
    ref[at + (0,)] = value[0]
    ref[at + (1,)] = value[1]


def loop(low, high, body, carry, by):
    by = by if (high - low) % by == 0 else 1

    def several(k, carry):
        for i in range(by):
            carry = body(low + k * by + i, carry)
        return carry

    return lax.fori_loop(0, (high - low) // by, several, carry)


def rotation(angles, shape):
    cos = [jnp.cos(jnp.full(shape, angles[i], jnp.float32)) for i in range(3)]
    sin = [jnp.sin(jnp.full(shape, angles[i], jnp.float32)) for i in range(3)]
    (ca, cb, cc), (sa, sb, sc) = cos, sin
    left = [[ca * cb, -sa, ca * sb], [sa * cb, ca, sa * sb], [-sb, jnp.zeros_like(cb), cb]]
    return [[row[0] * cc + row[1] * sc, row[1] * cc - row[0] * sc, row[2]] for row in left]


def relax(
    ngz,
    nxy,
    field,
    source,
    classes,
    boundary,
    conductance,
    angles,
    strengths,
    OUT,
    U,
    S,
    C,
    B,
    SG,
    DR,
    PH,
    PHI,
    PSI,
    T,
    QM,
    EPHI,
    EPSI,
    EH,
    ET,
    ends,
    coef,
    near,
    halo_out,
    halo_in,
    value_in,
    info_in,
    info_out,
    lam_in,
    lam_out,
    extra_in,
    extra_out,
    own_in,
    own_out,
    ch_in,
    ch_out,
    in_sems,
    halo_send,
    halo_recv,
    info_send,
    info_recv,
    lam_send,
    lam_recv,
    extra_send,
    extra_recv,
    own_send,
    own_recv,
    ch_send,
    ch_recv,
):
    ix, iz = lax.axis_index("xy"), lax.axis_index("gz")
    depth, _, _, rows, width = U.shape
    kinds = conductance.shape[0]
    plane = (rows, width)
    has = {
        ("xy", 0): ix > 0,
        ("xy", 1): ix < nxy - 1,
    }
    where_is = {
        ("xy", 0): ix - 1,
        ("xy", 1): ix + 1,
    }
    for steps in (1, 2):
        has["gz", -steps] = iz >= steps
        has["gz", steps] = iz < ngz - steps
        where_is["gz", -steps] = iz - steps
        where_is["gz", steps] = iz + steps
    zs = depth // PIECES
    spans = [pl.ds(piece * zs, zs) for piece in range(PIECES)]
    moves = [(field.at[span], U.at[span]) for span in spans]
    moves += [(classes, C), (boundary, B), (source, S)]
    loads = [
        pltpu.make_async_copy(src, dst, in_sems.at[i]) for i, (src, dst) in enumerate(moves)
    ]
    for load in loads[:-1]:
        load.start()

    barrier = pltpu.get_barrier_semaphore()
    for key, there in has.items():

        @pl.when(there)
        def _():
            pl.semaphore_signal(
                barrier,
                inc=1,
                device_id={key[0]: where_is[key]},
                device_id_type=pl.DeviceIdType.MESH,
            )


    def remote(src, dst, send, recv, key):
        return pltpu.make_async_remote_copy(
            src_ref=src,
            dst_ref=dst,
            send_sem=send,
            recv_sem=recv,
            device_id={key[0]: where_is[key]},
            device_id_type=pl.DeviceIdType.MESH,
        )

    def halo_copy(sweep, side, piece):
        span = pl.ds(piece * zs, zs)
        return remote(
            halo_out.at[sweep, side, :, :, span],
            halo_in.at[sweep, side, :, :, span],
            halo_send.at[sweep, side, piece],
            halo_recv.at[sweep, side, piece],
            ("xy", 1 - side),
        )

    def send_halo(sweep, piece):
        for side in range(2):

            @pl.when(has["xy", 1 - side])
            def _():
                halo_copy(sweep, side, piece).start()

    def pack(first, last, z, values):
        for i in range(6):
            at = (i // 3, i % 3, pl.ds(z, 1), slice(None))
            first[at] = values[i][:1, :]
            last[at] = values[i][rows - 1 :, :]

    for side in range(2):

        @pl.when(jnp.logical_not(has["xy", side]))
        def _():
            for sweep in range(SWEEPS):
                halo_in[sweep, side] = jnp.zeros(halo_in.shape[2:], jnp.float32)

        @pl.when((iz if side == 0 else ngz - 1 - iz) < 2)
        def _():
            for part in range(3, 9):
                info_in[side, part] = jnp.zeros(info_in.shape[2:], jnp.float32)
            extra_in[side] = jnp.zeros(extra_in.shape[1:], jnp.float32)
            lam_in[side] = jnp.zeros(lam_in.shape[1:], jnp.float32)
            for sweep in range(SWEEPS):
                for j in range(3):
                    ch_in[sweep, side, j] = jnp.zeros(ch_in.shape[3:], jnp.float32)

    count = sum(there.astype(jnp.int32) for there in has.values())

    def pack_first(z, carry):
        values = [U[z, i // 3, i % 3] for i in range(6)]
        pack(halo_out.at[0, 1], halo_out.at[0, 0], z, values)
        return carry

    for piece in range(PIECES):
        loads[piece].wait()
        if piece == PIECES - 1:
            loads[-1].start()
        loop(piece * zs, (piece + 1) * zs, pack_first, 0, 4)
        if piece == 0:
            pl.semaphore_wait(barrier, count)
        send_halo(0, piece)

    loads[PIECES].wait()
    loads[PIECES + 1].wait()

    def diagonal(z, carry):
        ids = C[z]
        sigma = jnp.zeros(plane, jnp.float32)
        for kind in range(kinds):
            sigma = jnp.where(ids == kind, conductance[kind], sigma)
        SG[z] = sigma
        DR[z] = 2.0 + 4.0 * coupling + penalty * B[z].astype(jnp.float32)
        return carry

    loop(0, depth, diagonal, 0, 4)

    def diag(z):
        real = jnp.broadcast_to(DR[z][None], (3,) + plane)
        sigma = SG[z]
        return real, jnp.stack([sigma * strengths[j] for j in range(3)])

    none = (jnp.zeros((3,) + plane, jnp.float32),) * 2

    def pivots(k, carry):
        p, q = carry
        z, back = k, depth - 1 - k
        d, f = diag(z), diag(back)
        p = inv((d[0] - p[0], d[1] - p[1]))
        q = inv((f[0] - q[0], f[1] - q[1]))
        put(PH, p, z)
        put(PHI, q, back)
        return p, q

    loop(0, depth, pivots, (none, none), 2)
    ones = (jnp.ones((3,) + plane, jnp.float32), none[0])

    def columns(k, carry):
        down, up = carry
        z, back = k, depth - 1 - k
        down = mul(get(PHI, z), down)
        up = mul(get(PH, back), up)
        put(PHI, down, z)
        put(PSI, up, back)
        return down, up

    loop(0, depth, columns, (ones, ones), 2)
    LEFT, RIGHT = 0, 1
    tip = (lambda: get(PHI, 0), lambda: get(PSI, depth - 1))
    across = lambda: get(PSI, 0)

    place = (iz, ngz - 1 - iz)
    even = [lax.rem(k, 2) == 0 for k in place]
    odd = [lax.rem(k, 2) == 1 for k in place]
    onward = [ngz - 1 - k for k in place]

    def to(side, steps):
        return {"gz": iz + steps if side == LEFT else iz - steps}

    def chain_copy(src, dst, send, recv, side, steps):
        return pltpu.make_async_remote_copy(
            src_ref=src,
            dst_ref=dst,
            send_sem=send,
            recv_sem=recv,
            device_id=to(side, steps),
            device_id_type=pl.DeviceIdType.MESH,
        )

    def info_copy(side, j):
        return chain_copy(
            info_out.at[side, j],
            info_in.at[side, j],
            info_send.at[side, j],
            info_recv.at[side, j],
            side,
            1,
        )

    def lam_copy(side, steps, j):
        return chain_copy(
            lam_out.at[side, j],
            lam_in.at[side, j],
            lam_send.at[side, steps - 1, j],
            lam_recv.at[side, j],
            side,
            steps,
        )

    def own_copy(sweep, side, j):
        return chain_copy(
            own_out.at[sweep, side, j],
            own_in.at[sweep, side, j],
            own_send.at[sweep, side, j],
            own_recv.at[sweep, side, j],
            side,
            1,
        )

    def x_copy(sweep, side, steps, j):
        return chain_copy(
            ch_out.at[sweep, side, j],
            ch_in.at[sweep, side, j],
            ch_send.at[sweep, side, steps - 1, j],
            ch_recv.at[sweep, side, j],
            side,
            steps,
        )

    both = jnp.logical_and

    def send_info(side):
        parts = (tip[1 - side](), tip[side](), across())
        for part in range(3):
            for j in range(3):
                for p in range(2):
                    info_out[side, part * 3 + j, p] = parts[part][p][j]
            sends = both(even[side], onward[side] >= 1)

            @pl.when(sends if part == 0 else both(sends, place[side] > 0))
            def _():
                for j in range(3):
                    info_copy(side, part * 3 + j).start()

    def pass_lam(side):
        @pl.when(odd[side])
        def _():
            for j in range(3):
                info_copy(side, j).wait_recv()

        @pl.when(both(odd[side], place[side] >= 2))
        def _():
            for j in range(3, 9):
                info_copy(side, j).wait_recv()

        @pl.when(place[side] >= 2)
        def _():
            for j in range(3):
                lam_copy(side, 1, j).wait_recv()

        for j in range(3):
            tips = [(info_in[side, 3 * k + j, 0], info_in[side, 3 * k + j, 1]) for k in range(3)]
            given = (lam_in[side, j, 0], lam_in[side, j, 1])

            @pl.when(odd[side])
            def _():
                skip = mul(tips[2], inv(one_minus(mul(tips[1], given))))
                along = mul(skip, given)
                lam = add(tips[0], mul(tips[2], along))
                for p in range(2):
                    coef[12 + side, p, j] = along[p]
                    coef[8 + side, p, j] = skip[p]
                    coef[10 + side, p, j] = lam[p]

            @pl.when(even[side])
            def _():
                for p in range(2):
                    coef[10 + side, p, j] = given[p]

            of = lambda pair: (pair[0][j], pair[1][j])
            lam = (coef[10 + side, 0, j], coef[10 + side, 1, j])
            kappa = mul(of(across()), inv(one_minus(mul(of(tip[side]()), lam))))
            over = mul(kappa, lam)
            value = add(of(tip[1 - side]()), mul(of(across()), over))
            for p in range(2):
                coef[side, p, j] = kappa[p]
                coef[2 + side, p, j] = over[p]
                lam_out[side, j, p] = value[p]

            @pl.when(both(odd[side], onward[side] >= 2))
            def _():
                lam_copy(side, 2, j).start()

        @pl.when(both(odd[side], onward[side] >= 1))
        def _():
            for j in range(3):
                lam_copy(side, 1, j).start()

    def extra_copy(side, j):
        return chain_copy(
            extra_out.at[side, j],
            extra_in.at[side, j],
            extra_send.at[side, j],
            extra_recv.at[side, j],
            side,
            1,
        )

    def own_base(side, j):
        return add(
            (ends[1 - side, 0, j], ends[1 - side, 1, j]),
            mul(
                (coef[2 + side, 0, j], coef[2 + side, 1, j]),
                (ends[side, 0, j], ends[side, 1, j]),
            ),
        )

    def own_sum(sweep, side):
        for j in range(3):
            if sweep == 0:
                for p in range(2):
                    own_out[sweep, side, j, p] = ends[1 - side, p, j]
                    extra_out[side, j, p] = ends[side, p, j]
            else:
                base = own_base(side, j)
                for p in range(2):
                    own_out[sweep, side, j, p] = base[p]
            sends = both(even[side], onward[side] >= 1)

            @pl.when(sends)
            def _():
                own_copy(sweep, side, j).start()

            if sweep == 0:

                @pl.when(both(sends, place[side] > 0))
                def _():
                    extra_copy(side, j).start()

    def pass_chain(sweep, side):
        for j in range(3):
            base = own_base(side, j)

            @pl.when(odd[side])
            def _():
                own_copy(sweep, side, j).wait_recv()

            if sweep == 0:

                @pl.when(both(odd[side], place[side] >= 2))
                def _():
                    extra_copy(side, j).wait_recv()

            @pl.when(place[side] >= 2)
            def _():
                x_copy(sweep, side, 1, j).wait_recv()

            given = (ch_in[sweep, side, j, 0], ch_in[sweep, side, j, 1])

            @pl.when(odd[side])
            def _():
                own = (own_in[sweep, side, j, 0], own_in[sweep, side, j, 1])
                if sweep == 0:
                    extra = (extra_in[side, j, 0], extra_in[side, j, 1])
                    own = add(own, mul((coef[12 + side, 0, j], coef[12 + side, 1, j]), extra))
                x = add(own, mul((coef[8 + side, 0, j], coef[8 + side, 1, j]), given))
                for p in range(2):
                    value_in[side, j, p] = x[p]

            @pl.when(even[side])
            def _():
                for p in range(2):
                    value_in[side, j, p] = given[p]

            x = (value_in[side, j, 0], value_in[side, j, 1])
            result = add(base, mul((coef[side, 0, j], coef[side, 1, j]), x))
            for p in range(2):
                ch_out[sweep, side, j, p] = result[p]

            @pl.when(both(odd[side], onward[side] >= 2))
            def _():
                x_copy(sweep, side, 2, j).start()

        @pl.when(both(odd[side], onward[side] >= 1))
        def _():
            for j in range(3):
                x_copy(sweep, side, 1, j).start()

    left_first = iz * 2 < ngz - 1

    def near_side(run):
        @pl.when(left_first)
        def _():
            run(LEFT)

        @pl.when(jnp.logical_not(left_first))
        def _():
            run(RIGHT)

    def far_side(run):
        @pl.when(left_first)
        def _():
            run(RIGHT)

        @pl.when(jnp.logical_not(left_first))
        def _():
            run(LEFT)

    near_side(send_info)
    far_side(send_info)

    angle_matrix = rotation(angles, (rows, 128))
    for c in range(3):
        for j in range(3):
            QM[c, j] = angle_matrix[c][j]

    def matrix():
        return [
            [jnp.concatenate([QM[c, j]] * (width // 128), axis=1) for j in range(3)]
            for c in range(3)
        ]

    def pack_columns(z, carry):
        for src, dst in ((PHI, EPHI), (PSI, EPSI)):
            pack(dst.at[0], dst.at[1], z, [src[z, i // 3, i % 3] for i in range(6)])
        return carry

    loop(0, depth, pack_columns, 0, 4)

    row = lax.broadcasted_iota(jnp.int32, plane, 0)
    lane = lax.broadcasted_iota(jnp.int32, plane, 1)
    zero = jnp.zeros(plane, jnp.float32)

    def turn(q, driven):
        return [
            jnp.stack(
                [
                    q[0][j] * driven[p][0] + q[1][j] * driven[p][1] + q[2][j] * driven[p][2]
                    for j in range(3)
                ]
            )
            for p in range(2)
        ]

    def inner(z, carry):
        first, last = carry
        q = matrix()
        driven = []
        for p in range(2):
            of = []
            for c in range(3):
                u = U[z, p, c]
                beside = jnp.where(lane == 0, zero, pltpu.roll(u, 1, 1))
                beside += jnp.where(lane == width - 1, zero, pltpu.roll(u, width - 1, 1))
                beside += jnp.where(row == 0, zero, pltpu.roll(u, 1, 0))
                beside += jnp.where(row == rows - 1, zero, pltpu.roll(u, rows - 1, 0))
                of.append(S[z, p, c] + coupling * beside)
            driven.append(of)
        turned = turn(q, driven)
        put(T, turned, z)
        return add(first, mul(get(PHI, z), turned)), add(last, mul(get(PSI, z), turned))

    tiles = [pl.ds(z, rows) for z in range(0, depth, rows)]

    def outer(sweep, side, tile, carry):
        first, last = carry
        q = matrix()
        turned = turn(
            q,
            [[coupling * halo_in[sweep, side, p, c, tile] for c in range(3)] for p in range(2)],
        )
        for p in range(2):
            EH[side, p, :, tile] = turned[p]
        phi = [EPHI[side, p, :, tile] for p in range(2)]
        psi = [EPSI[side, p, :, tile] for p in range(2)]
        return add(first, mul(phi, turned)), add(last, mul(psi, turned))

    loads[PIECES + 2].wait()
    for sweep in range(SWEEPS):
        sums = loop(0, depth, inner, (none, none), 4)
        if sweep == 0:
            near_side(pass_lam)
        halves = [(none, none), (none, none)]
        for piece in range(PIECES):
            for side in range(2):

                @pl.when(has["xy", side])
                def _():
                    halo_copy(sweep, side, piece).wait_recv()

                for tile in tiles[piece * len(tiles) // PIECES : (piece + 1) * len(tiles) // PIECES]:
                    halves[side] = outer(sweep, side, tile, halves[side])
        for side in range(2):
            here = row == (0 if side == 0 else rows - 1)
            sums = tuple(
                add(
                    sums[end],
                    tuple(
                        jnp.where(here[None], jnp.sum(part, axis=1, keepdims=True), 0.0)
                        for part in halves[side][end]
                    ),
                )
                for end in range(2)
            )
        put(ends, sums[0], 0)
        put(ends, sums[1], 1)

        near_side(functools.partial(own_sum, sweep))
        far_side(functools.partial(own_sum, sweep))
        near_side(functools.partial(pass_chain, sweep))

        def forward(z, m):
            given = []
            for p in range(2):
                edges = []
                for j in range(3):
                    above = jnp.broadcast_to(EH[0, p, j, pl.ds(z, 1), :], plane)
                    below = jnp.broadcast_to(EH[1, p, j, pl.ds(z, 1), :], plane)
                    edges.append(
                        jnp.where(row == 0, above, zero) + jnp.where(row == rows - 1, below, zero)
                    )
                given.append(T[z, p] + jnp.stack(edges))
            m = mul(get(PH, z), add(given, m))
            put(T, m, z)
            return m

        def backward(k, w):
            z = depth - 1 - k
            w = add(get(T, z), mul(get(PH, z), w))
            put(T, w, z)
            if sweep < SWEEPS - 1:
                pack(ET.at[0], ET.at[1], z, [w[i // 3][i % 3] for i in range(6)])
            return w

        loop(0, depth, forward, none, 4)
        loop(0, depth, backward, none, 4)
        if sweep == 0:
            far_side(pass_lam)
            for side in range(2):
                lam = get(coef, 10 + side)
                away = tuple(
                    jnp.stack([lam_out[1 - side, j, p] for j in range(3)]) for p in range(2)
                )
                det = inv(one_minus(mul(lam, away)))
                put(coef, det, 6 + side)
                put(coef, mul(det, lam), 4 + side)
        far_side(functools.partial(pass_chain, sweep))

        for side in range(2):
            for j in range(3):
                arrived = (value_in[side, j, 0], value_in[side, j, 1])
                other = (ch_out[sweep, 1 - side, j, 0], ch_out[sweep, 1 - side, j, 1])
                value = add(
                    mul((coef[6 + side, 0, j], coef[6 + side, 1, j]), arrived),
                    mul((coef[4 + side, 0, j], coef[4 + side, 1, j]), other),
                )
                near[side, 0, j] = value[0]
                near[side, 1, j] = value[1]

        final = sweep == SWEEPS - 1

        def join_edge(side, tile):
            q = matrix()
            r = 0 if side == 0 else rows - 1
            w = [ET[side, p, :, tile] for p in range(2)]
            for end, column in ((0, EPHI), (1, EPSI)):
                entry = [
                    jnp.broadcast_to(near[end, p, :, r : r + 1, :], (3,) + plane)
                    for p in range(2)
                ]
                w = add(w, mul([column[side, p, :, tile] for p in range(2)], entry))
            for p in range(2):
                for c in range(3):
                    halo_out[sweep + 1, 1 - side, p, c, tile] = (
                        q[c][0] * w[p][0] + q[c][1] * w[p][1] + q[c][2] * w[p][2]
                    )

        if not final:
            for piece in range(PIECES):
                for tile in tiles[piece * len(tiles) // PIECES : (piece + 1) * len(tiles) // PIECES]:
                    for side in range(2):
                        join_edge(side, tile)
                send_halo(sweep + 1, piece)


        def join(z, carry):
            q = matrix()
            before, after = get(near, 0), get(near, 1)
            w = add(add(get(T, z), mul(get(PHI, z), before)), mul(get(PSI, z), after))
            values = []
            for p in range(2):
                for c in range(3):
                    values.append(q[c][0] * w[p][0] + q[c][1] * w[p][1] + q[c][2] * w[p][2])
            target = OUT if final else U
            for i in range(6):
                target[z, i // 3, i % 3] = values[i]
            return carry

        loop(0, depth, join, 0, 4)

    for side in range(2):

        @pl.when(has["xy", 1 - side])
        def _():
            for sweep in range(SWEEPS):
                for piece in range(PIECES):
                    halo_copy(sweep, side, piece).wait_send()

        sends = both(even[side], onward[side] >= 1)

        @pl.when(sends)
        def _():
            for j in range(3):
                info_copy(side, j).wait_send()
                for sweep in range(SWEEPS):
                    own_copy(sweep, side, j).wait_send()

        @pl.when(both(sends, place[side] > 0))
        def _():
            for j in range(3, 9):
                info_copy(side, j).wait_send()
            for j in range(3):
                extra_copy(side, j).wait_send()

        for steps in (2, 1):

            @pl.when(both(odd[side], onward[side] >= steps))
            def _():
                for j in range(3):
                    lam_copy(side, steps, j).wait_send()
                    for sweep in range(SWEEPS):
                        x_copy(sweep, side, steps, j).wait_send()


def local(ngz, nxy, field, source, classes, boundary, conductance, angles, strengths):
    depth, _, _, rows, width = field.shape
    f32 = jnp.float32
    block = pltpu.VMEM(field.shape, f32)
    flat = (depth, rows, width)
    line = (2, 3, rows, width)
    pair = (2, rows, width)
    edge = (2, 2, 3, depth, width)
    dma = pltpu.SemaphoreType.DMA
    hbm = pl.BlockSpec(memory_space=pl.ANY)
    smem = pl.BlockSpec(memory_space=pltpu.SMEM)
    return pl.pallas_call(
        functools.partial(relax, ngz, nxy),
        out_shape=pltpu.VMEM(field.shape, f32),
        in_specs=[hbm] * 4 + [smem] * 3,
        out_specs=pl.BlockSpec(memory_space=pltpu.VMEM),
        scratch_shapes=[
            block,
            block,
            pltpu.VMEM(flat, jnp.int32),
            pltpu.VMEM(flat, jnp.int32),
            pltpu.VMEM(flat, f32),
            pltpu.VMEM(flat, f32),
            block,
            block,
            block,
            block,
            pltpu.VMEM((3, 3, rows, 128), f32),
            pltpu.VMEM(edge, f32),
            pltpu.VMEM(edge, f32),
            pltpu.VMEM(edge, f32),
            pltpu.VMEM(edge, f32),
            pltpu.VMEM((2,) + line, f32),
            pltpu.VMEM((14,) + line, f32),
            pltpu.VMEM((2,) + line, f32),
            pltpu.VMEM((SWEEPS,) + edge, f32),
            pltpu.VMEM((SWEEPS,) + edge, f32),
            pltpu.VMEM((2, 3) + pair, f32),
            pltpu.VMEM((2, 9) + pair, f32),
            pltpu.VMEM((2, 9) + pair, f32),
            pltpu.VMEM((2, 3) + pair, f32),
            pltpu.VMEM((2, 3) + pair, f32),
            pltpu.VMEM((2, 3) + pair, f32),
            pltpu.VMEM((2, 3) + pair, f32),
            pltpu.VMEM((SWEEPS, 2, 3) + pair, f32),
            pltpu.VMEM((SWEEPS, 2, 3) + pair, f32),
            pltpu.VMEM((SWEEPS, 2, 3) + pair, f32),
            pltpu.VMEM((SWEEPS, 2, 3) + pair, f32),
            dma((PIECES + 3,)),
            dma((SWEEPS, 2, PIECES)),
            dma((SWEEPS, 2, PIECES)),
            dma((2, 9)),
            dma((2, 9)),
            dma((2, 2, 3)),
            dma((2, 3)),
            dma((2, 3)),
            dma((2, 3)),
            dma((SWEEPS, 2, 3)),
            dma((SWEEPS, 2, 3)),
            dma((SWEEPS, 2, 2, 3)),
            dma((SWEEPS, 2, 3)),
        ],
        compiler_params=pltpu.CompilerParams(collective_id=0, has_side_effects=True, vmem_limit_bytes=VMEM_LIMIT),
    )(field, source, classes, boundary, conductance, angles, strengths)


def solution(mesh):
    in_specs = (
        P("gz", None, None, "xy", None),
        P("gz", None, None, "xy", None),
        P("gz", "xy", None),
        P("gz", "xy", None),
        P(),
        P(),
        P(),
    )
    out_specs = P("gz", None, None, "xy", None)
    body = functools.partial(local, mesh.shape["gz"], mesh.shape["xy"])
    return jax.shard_map(body, mesh=mesh, in_specs=in_specs, out_specs=out_specs, check_vma=False)
```
